16 devices in a mesh: rep: 1, r: 2 (over z), s: 8 (over x, y, core).
Axes of the slice: x: 2, y: 2, z: 2, core: 2. Of those that a mesh axis runs over, the one named last changes fastest.
Arguments:
- x: bfloat16 [16, 2048, 896], P(('rep', 'r', 's'))
- dy: bfloat16 [16, 2048, 896], P(('rep', 'r', 's'))
- w_gate: bfloat16 [2, 896, 3584], P(None, 's')
- w_up: bfloat16 [2, 896, 3584], P(None, 's')
- w_down: bfloat16 [2, 3584, 896], P(None, 's')
- m_w_gate: float32 [2, 896, 3584], P(None, 's')
- m_w_up: float32 [2, 896, 3584], P(None, 's')
- m_w_down: float32 [2, 3584, 896], P(None, 's')
- v_w_gate: float32 [2, 896, 3584], P(None, 's')
- v_w_up: float32 [2, 896, 3584], P(None, 's')
- v_w_down: float32 [2, 3584, 896], P(None, 's')
Outputs:
- output 1: bfloat16 [2, 896, 3584], P('rep', 's')
- output 2: bfloat16 [2, 896, 3584], P('rep', 's')
- output 3: bfloat16 [2, 3584, 896], P('rep', 's')
- output 4: float32 [2, 896, 3584], P('rep', 's')
- output 5: float32 [2, 896, 3584], P('rep', 's')
- output 6: float32 [2, 3584, 896], P('rep', 's')
- output 7: float32 [2, 896, 3584], P('rep', 's')
- output 8: float32 [2, 896, 3584], P('rep', 's')
- output 9: float32 [2, 3584, 896], P('rep', 's')
All inputs are finite; a program needn't handle non-finite values.
Results may differ from the reference program's by a relative error of at most 0.022.
Values are sent between devices in bfloat16 or wider.
A program may use at most 2 GiB of HBM per device.

```python
import jax
import jax.numpy as jnp
from jax import lax

SEQUENCES = 16
TOKENS = 2048
D = 896
FF = 3584
LAYERS = 2
NAMES = ("w_gate", "w_up", "w_down")
SHAPES = {"w_gate": (LAYERS, D, FF), "w_up": (LAYERS, D, FF), "w_down": (LAYERS, FF, D)}


def bump(key, n, height):
    away = (jnp.arange(n, dtype=jnp.int32) - jax.random.randint(key, (), 0, n, jnp.int32)) % n
    return jnp.where(away < n // 8, height, 1.0)


def together(key, own, strength):
    shared = jax.random.normal(key, own.shape[1:], jnp.float32)
    return (own + strength * shared) * lax.rsqrt(1 + strength * strength)


def setup_inputs(seed: int = 0, part: int = 0) -> dict:
    kx, kdy, ka, kb, kz, kf, kh, kl, *keys = jax.random.split(jax.random.key(seed), 8 + 3 * len(NAMES))
    kx, kdy, ka, kb = (jax.random.fold_in(k, part) for k in (kx, kdy, ka, kb))
    kw, km, kv = (keys[i::3] for i in range(3))
    shape = (SEQUENCES, TOKENS, D)
    much_x, much_dy = jax.random.uniform(kz, (2,), jnp.float32, 0.0, 1.0)
    loud = 2.0 ** jax.random.uniform(jax.random.fold_in(kz, 1), (), jnp.float32, -1.0, 2.0)
    layers = 2.0 ** jax.random.uniform(kl, (LAYERS, 1, 1), jnp.float32, -1.0, 1.0)
    x = together(ka, jax.random.normal(kx, shape, jnp.float32), much_x) * bump(kf, D, 4.0)
    dy = together(kb, jax.random.normal(kdy, shape, jnp.float32), much_dy)
    drawn = {"x": x.astype(jnp.bfloat16), "dy": (loud * dy * (SEQUENCES * TOKENS) ** -0.5).astype(jnp.bfloat16)}
    for key, name in zip(kw, NAMES, strict=True):
        w = jax.random.normal(key, SHAPES[name], jnp.float32) * SHAPES[name][1] ** -0.5
        drawn[name] = (w * {"w_gate": 1.0, "w_up": bump(kh, FF, 4.0), "w_down": layers}[name]).astype(jnp.bfloat16)
    for key, name in zip(km, NAMES, strict=True):
        drawn[f"m_{name}"] = 0.1 * jax.random.normal(key, SHAPES[name], jnp.float32)
    for key, name in zip(kv, NAMES, strict=True):
        drawn[f"v_{name}"] = jax.random.uniform(key, SHAPES[name], jnp.float32, 0.005, 0.015)
    return drawn


def matmul(a, w):
    return jnp.dot(a, w, preferred_element_type=jnp.float32).astype(jnp.bfloat16)


def normed(h):
    wide = h.astype(jnp.float32)
    scale = lax.rsqrt(jnp.mean(wide**2, -1, keepdims=True) + 1e-6)
    return (wide * scale).astype(jnp.bfloat16)


def layer(h, w):
    a = normed(h)
    gate = jnp.dot(a, w["w_gate"], preferred_element_type=jnp.float32)
    up = jnp.dot(a, w["w_up"], preferred_element_type=jnp.float32)
    return h + matmul((jax.nn.silu(gate) * up).astype(jnp.bfloat16), w["w_down"])


def adamw(w, m, v, g):
    m = 0.9 * m + 0.1 * g
    v = 0.95 * v + 0.05 * g * g
    step = m * lax.rsqrt(v + 1e-8) + 0.1 * w
    return (w - 0.02 * step).astype(jnp.bfloat16), m, v


def clipped(gradients, sum_of_squares, count):
    factor = jnp.minimum(1.0, 0.5 * lax.rsqrt(sum_of_squares / count + 1e-30))
    return [g * factor for g in gradients]


def stack(weights, h):
    return lax.scan(lambda h, w: (layer(h, w), None), h, weights)[0]


def reference(x, dy, w_gate, w_up, w_down, m_w_gate, m_w_up, m_w_down, v_w_gate, v_w_up, v_w_down):
    weights = dict(zip(NAMES, (w_gate, w_up, w_down), strict=True))

    def take(so_far, sequence):
        h, by_y = sequence
        _, back = jax.vjp(lambda w: stack(w, h), weights)
        return jax.tree.map(lambda total, term: total + term.astype(jnp.float32), so_far, back(by_y)[0]), None

    none_yet = {name: jnp.zeros(w.shape, jnp.float32) for name, w in weights.items()}
    by_weights, _ = lax.scan(take, none_yet, (x, dy))
    gradients = [by_weights[name].astype(jnp.bfloat16).astype(jnp.float32) for name in NAMES]
    gradients = clipped(gradients, sum(jnp.sum(g * g) for g in gradients), sum(g.size for g in gradients))
    new = [
        adamw(w.astype(jnp.float32), m, v, g)
        for w, m, v, g in zip((w_gate, w_up, w_down), (m_w_gate, m_w_up, m_w_down), (v_w_gate, v_w_up, v_w_down), gradients, strict=True)
    ]
    return tuple(one[which] for which in range(3) for one in new)
```

```python
import jax
import jax.numpy as jnp
from jax import lax
from jax.experimental import pallas as pl
from jax.experimental.pallas import tpu as pltpu
from jax.sharding import PartitionSpec as P

MESH = pl.DeviceIdType.MESH
T, D, FF = 2048, 896, 3584
TILES, WIDE, ROWS = 7, 512, 512
BLOCKS = T // ROWS
STEPS = 2 * TILES
F32, BF16 = jnp.float32, jnp.bfloat16
VMEM_LIMIT = 67_043_328
ANY = pl.BlockSpec(memory_space=pl.ANY)


def dot(a, b, contract=(1, 0)):
    return lax.dot_general(a, b, (((contract[0],), (contract[1],)), ((), ())), preferred_element_type=F32)


def normed(h):
    wide = h.astype(F32)
    scale = lax.rsqrt(jnp.mean(wide**2, -1, keepdims=True) + 1e-6)
    return (wide * scale).astype(BF16)


def block(i):
    return pl.ds(pl.multiple_of(i * ROWS, ROWS), ROWS)


class Place:
    def __init__(self):
        r, s = lax.axis_index("r"), lax.axis_index("s")
        c, q = s % 2, s // 2
        y, x = q % 2, q // 2
        self.r, self.s, self.c, self.q = r, s, c, q
        dx, dy = 2 - 4 * x, 1 - 2 * y
        self.qx, self.qy, self.qd = q + dx, q + dy, q + dx + dy
        self.sx, self.sy, self.sc = s + 2 * dx, s + 2 * dy, s + 1 - 2 * c
        self.sd = s + 2 * dx + 2 * dy
        self.sa = self.sx + r * (self.sy - self.sx)
        self.sb = self.sy + r * (self.sx - self.sy)
        self.to_a, self.to_b = {"s": self.sa}, {"s": self.sb}
        self.to_x, self.to_y, self.to_c, self.to_z = {"s": self.sx}, {"s": self.sy}, {"s": self.sc}, {"r": 1 - r}


def barrier(at):
    sem = pltpu.get_barrier_semaphore()
    for to in (at.to_x, at.to_y, at.to_c, at.to_z):
        pl.semaphore_signal(sem, inc=1, device_id=to, device_id_type=MESH)
    pl.semaphore_wait(sem, 4)


class Gather:
    def __init__(self, at, piece, send, recv):
        self.at, self.piece, self.send, self.recv = at, piece, send, recv

    def copy(self, way, n, shard, to):
        ref = self.piece(n, shard)
        return pltpu.make_async_remote_copy(
            src_ref=ref, dst_ref=ref, send_sem=self.send.at[way, n], recv_sem=self.recv.at[way, n], device_id=to, device_id_type=MESH
        )

    def own(self, n):
        self.copy(0, n, self.at.s, self.at.to_a).start()
        self.copy(3, n, self.at.s, self.at.to_c).start()

    def first(self, n):
        at = self.at
        self.copy(0, n, at.sa, at.to_a).wait_recv()
        self.copy(1, n, at.sa, at.to_z).start()
        self.copy(2, n, at.sa, at.to_b).start()
        self.copy(4, n, at.sa, at.to_c).start()

    def second(self, n):
        at = self.at
        self.copy(1, n, at.sb, at.to_z).wait_recv()
        self.copy(5, n, at.sb, at.to_c).start()
        self.copy(2, n, at.sd, at.to_b).wait_recv()
        self.copy(6, n, at.sd, at.to_c).start()

    def whole(self, n):
        at = self.at
        across = at.sc - at.s
        for way, shard in ((3, at.s), (4, at.sa), (5, at.sb), (6, at.sd)):
            self.copy(way, n, shard + across, at.to_c).wait_recv()

    def sent(self, n):
        at = self.at
        for way, shard, to in (
            (0, at.s, at.to_a), (1, at.sa, at.to_z), (2, at.sa, at.to_b),
            (3, at.s, at.to_c), (4, at.sa, at.to_c), (5, at.sb, at.to_c), (6, at.sd, at.to_c),
        ):
            self.copy(way, n, shard, to).wait_send()


def load_own(at, layer, wg_h, wu_h, wd_h, WGU, WD, own):
    for i in range(TILES):
        for which, w in enumerate((wg_h, wu_h)):
            for k in range(4):
                pltpu.make_async_copy(
                    w.at[layer, :, pl.ds(k * 896 + i * 128, 128)], WGU.at[i, which, at.s, :, pl.ds(k * 128, 128)], own.at[i]
                ).start()
    pltpu.make_async_copy(wd_h.at[layer], WD.at[at.q, pl.ds(at.c * 7, 7)], own.at[TILES]).start()


def wait_own_tile(at, i, WGU, own):
    pltpu.make_async_copy(WGU.at[i, :, at.s], WGU.at[i, :, at.s], own.at[i]).wait()


def wait_own_down(at, wd_h, layer, WD, own):
    pltpu.make_async_copy(wd_h.at[layer], WD.at[at.q, pl.ds(at.c * 7, 7)], own.at[TILES]).wait()


def gathers(at, WGU, WD, sgu, rgu, sd, rd):
    gu = Gather(at, lambda n, s: WGU.at[n, :, s], sgu, rgu)
    down = Gather(at, lambda n, s: WD.at[s // 2, (s % 2) * 7 + n], sd, rd)
    return gu, down


def gate_up(WGU, i, which):
    return WGU[i, which].reshape(D, WIDE)


def down_tile(WD, i):
    return WD[:, pl.ds(2 * i, 2)].reshape(WIDE, D)


def forward_kernel(
    x_h, wg_h, wu_h, wd_h,
    gu_o, a0t_o, h1_o, a1_o, a1t_o, wd_o,
    WGU, WD, X, A, AT, MID, ST,
    load, own, stage, out, sgu, rgu, sd, rd,
):
    at = Place()
    load_own(at, 0, wg_h, wu_h, wd_h, WGU, WD, own)
    x_in = pltpu.make_async_copy(x_h, X, load)
    x_in.start()
    barrier(at)
    gu, down = gathers(at, WGU, WD, sgu, rgu, sd, rd)

    def start_tile(n, _):
        wait_own_tile(at, n, WGU, own)
        gu.own(n)
        return 0

    lax.fori_loop(0, TILES, start_tile, 0)
    wait_own_down(at, wd_h, 0, WD, own)
    lax.fori_loop(0, TILES, lambda n, _: (down.own(n), 0)[1], 0)
    x_in.wait()

    def norm(m, _):
        a = normed(X[block(m), :])
        A[block(m), :] = a
        AT[:, :, block(m)] = a.T.reshape(2, 448, ROWS)
        return 0

    lax.fori_loop(0, BLOCKS, norm, 0)
    a0t_out = pltpu.make_async_copy(AT, a0t_o, out.at[0])
    a0t_out.start()
    gu.first(0)

    def staged(i, m, slot):
        return pltpu.make_async_copy(ST.at[slot], gu_o.at[i, :, block(m), :], stage.at[slot])

    def tile(i, _):
        pl.when(i < TILES - 1)(lambda: gu.first(i + 1))
        gu.second(i)
        gu.whole(i)

        def rows(m, _):
            slot = m % 2
            pl.when(i * BLOCKS + m >= 2)(lambda: staged(i, m, slot).wait())
            a = A[block(m), :]
            gate = dot(a, gate_up(WGU, i, 0))
            up = dot(a, gate_up(WGU, i, 1))
            ST[slot, 0] = gate
            ST[slot, 1] = up
            staged(i, m, slot).start()
            MID[i, block(m), :] = (gate * jax.nn.sigmoid(gate) * up).astype(BF16)
            return 0

        return lax.fori_loop(0, BLOCKS, rows, 0)

    lax.fori_loop(0, TILES, tile, 0)
    down.first(0)

    def piece(n, _):
        pl.when(n < TILES - 1)(lambda: down.first(n + 1))
        down.second(n)
        down.whole(n)
        return 0

    lax.fori_loop(0, TILES, piece, 0)
    wd_out = pltpu.make_async_copy(WD, wd_o, out.at[1])
    wd_out.start()
    a0t_out.wait()

    def finish(m, _):
        total = dot(MID[0, block(m), :], down_tile(WD, 0))
        for i in range(1, TILES):
            total += dot(MID[i, block(m), :], down_tile(WD, i))
        h = (X[block(m), :].astype(F32) + total.astype(BF16).astype(F32)).astype(BF16)
        X[block(m), :] = h
        a = normed(h)
        A[block(m), :] = a
        AT[:, :, block(m)] = a.T.reshape(2, 448, ROWS)
        return 0

    lax.fori_loop(0, BLOCKS, finish, 0)
    outs = [pltpu.make_async_copy(v, o, out.at[2 + k]) for k, (v, o) in enumerate(((X, h1_o), (A, a1_o), (AT, a1t_o)))]
    for o in outs:
        o.start()
    for slot in range(2):
        staged(TILES - 1, slot, slot).wait()

    def sent(n, _):
        gu.sent(n)
        down.sent(n)
        return 0

    lax.fori_loop(0, TILES, sent, 0)
    wd_out.wait()
    for o in outs:
        o.wait()


def added(a, b):
    return (a.astype(F32) + b.astype(F32)).astype(BF16)


def backward_kernel(
    a1_h, a1t_h, h1_h, dy_h, a0t_h, gu_h, wd0_h, wg_h, wu_h, wd_h,
    gg_o, gu_o, gd_o, sqw_o, sqd_o,
    WGU, WD, A, AT, DY, ACC, MID, DG, DU, TW, TD, RW, RD, FW, FD, BW, BD, ZW, ZD, OW, OD,
    load, own, gus, sgu, rgu, sd, rd, pair_s, pair_r, first_s, first_r, second_s, second_r, z_s, z_r, ow_s, od_s, od_remote_s, od_r,
    pair_free, first_x, first_y, second_x, second_y, z_free,
):
    at = Place()
    c, q, qx, qy, qd = at.c, at.q, at.qx, at.qy, at.qd
    load_own(at, 1, wg_h, wu_h, wd_h, WGU, WD, own)
    loads = [pltpu.make_async_copy(h, v, load.at[k]) for k, (h, v) in enumerate(((a1_h, A), (a1t_h, AT), (dy_h, DY)))]
    for one in loads:
        one.start()
    h1_in = pltpu.make_async_copy(h1_h, A, load.at[0])
    wd0_in = pltpu.make_async_copy(wd0_h, WD, load.at[2])
    a0t_in = pltpu.make_async_copy(a0t_h, AT, load.at[1])
    barrier(at)
    gather, down = gathers(at, WGU, WD, sgu, rgu, sd, rd)
    wait_own_down(at, wd_h, 1, WD, own)
    lax.fori_loop(0, TILES, lambda n, _: (down.own(n), 0)[1], 0)

    def start_tile(n, _):
        wait_own_tile(at, n, WGU, own)
        gather.own(n)
        return 0

    lax.fori_loop(0, TILES, start_tile, 0)
    sqw_o[...] = jnp.zeros_like(sqw_o)
    sqd_o[...] = jnp.zeros_like(sqd_o)
    down.first(0)

    def piece(n, _):
        pl.when(n < TILES - 1)(lambda: down.first(n + 1))
        down.second(n)
        return 0

    lax.fori_loop(0, TILES, piece, 0)
    gather.first(0)
    lax.fori_loop(0, TILES, lambda n, _: (down.whole(n), 0)[1], 0)
    gather.second(0)
    for one in loads:
        one.wait()

    def remote(src, dst, send, recv, to):
        return pltpu.make_async_remote_copy(src_ref=src, dst_ref=dst, send_sem=send, recv_sem=recv, device_id=to, device_id_type=MESH)

    def credit(sem, to):
        pl.semaphore_signal(sem, inc=1, device_id=to, device_id_type=MESH)

    def pair_copies(t):
        k, j = t % 3, t % 2
        return [
            remote(TW.at[k, :, :, 1 - c], RW.at[j], pair_s.at[0, j], pair_r.at[0, j], at.to_c),
            remote(TD.at[k, :, 1 - c], RD.at[j], pair_s.at[1, j], pair_r.at[1, j], at.to_c),
        ]

    def pair_send(t):
        pl.when(t >= 2)(lambda: pl.semaphore_wait(pair_free, 1))
        for one in pair_copies(t):
            one.start()

    def pair_add(t):
        k, j = t % 3, t % 2
        for one in pair_copies(t):
            one.wait()

        def chip(p, _):
            for which in range(2):
                TW[k, which, p, c] = added(TW[k, which, p, c], RW[j, which, p])
            TD[k, p, c] = added(TD[k, p, c], RD[j, p])
            return 0

        lax.fori_loop(0, 4, chip, 0)
        pl.when(t < STEPS - 2)(lambda: credit(pair_free, at.to_c))

    def ways(t):
        turn = t % 2
        x, y = (at.sx, qx), (at.sy, qy)
        mixed = tuple(a + turn * (b - a) for a, b in zip(x, y))
        other = tuple(b + turn * (a - b) for a, b in zip(x, y))
        return (x, y), (y, x), (mixed, other)

    def buffers(t, which):
        k, j = t % 3, t % 2
        if which < 2:
            return (lambda p: TW.at[k, which, p, c]), (lambda n: FW.at[j, which, n]), BW.at[j, which]
        return (lambda p: TD.at[k, p, c]), (lambda n: FD.at[j, n]), BD.at[j]

    def first_copies(t):
        j, copies = t % 2, []
        for which, (one, _) in enumerate(ways(t)):
            mine, into, _ = buffers(t, which)
            for n, p in enumerate((one[1], qd)):
                copies.append(remote(mine(p), into(n), first_s.at[2 * which + n, j], first_r.at[2 * which + n, j], {"s": one[0]}))
        return copies

    def first_send(t):
        @pl.when(t >= 2)
        def _():
            pl.semaphore_wait(first_x, 1)
            pl.semaphore_wait(first_y, 1)

        for one in first_copies(t):
            one.start()

    def first_add(t):
        for one in first_copies(t):
            one.wait()
        for which, (_, two) in enumerate(ways(t)):
            mine, into, _ = buffers(t, which)
            for n, p in enumerate((q, two[1])):
                mine(p)[...] = added(mine(p)[...], into(n)[...])

        @pl.when(t < STEPS - 2)
        def _():
            credit(first_x, at.to_x)
            credit(first_y, at.to_y)

    def second_copies(t):
        j, copies = t % 2, []
        for which, (_, two) in enumerate(ways(t)):
            mine, _, into = buffers(t, which)
            copies.append(remote(mine(two[1]), into, second_s.at[which, j], second_r.at[which, j], {"s": two[0]}))
        return copies

    def second_send(t):
        @pl.when(t >= 2)
        def _():
            pl.semaphore_wait(second_x, 1)
            pl.semaphore_wait(second_y, 1)

        for one in second_copies(t):
            one.start()

    def second_add(t):
        for one in second_copies(t):
            one.wait()
        for which in range(3):
            mine, _, into = buffers(t, which)
            mine(q)[...] = added(mine(q)[...], into[...])

        @pl.when(t < STEPS - 2)
        def _():
            credit(second_x, at.to_x)
            credit(second_y, at.to_y)

    def z_copies(t):
        k, j = t % 3, t % 2
        return [
            remote(TW.at[k, :, q, c], ZW.at[j], z_s.at[0, j], z_r.at[0, j], at.to_z),
            remote(TD.at[k, q, c], ZD.at[j], z_s.at[1, j], z_r.at[1, j], at.to_z),
        ]

    def z_send(t):
        pl.when(t >= 2)(lambda: pl.semaphore_wait(z_free, 1))
        for one in z_copies(t):
            one.start()

    def half(t, core):
        number = (t % TILES) * 2 + core
        return number // 7, number % 7

    def layer_of(t):
        return 1 - t // TILES

    def wide_out(t):
        j, i = t % 2, t % TILES
        for which, o in enumerate((gg_o, gu_o)):
            for k in range(4):
                lanes = pl.ds(pl.multiple_of(k * 896 + i * 128, 128), 128)
                yield pltpu.make_async_copy(OW.at[j, which, :, pl.ds(k * 128, 128)], o.at[layer_of(t), :, lanes], ow_s.at[j])

    def down_local(t):
        _, number = half(t, c)
        return pltpu.make_async_copy(OD.at[t % 2], gd_o.at[layer_of(t), number], od_s.at[t % 2])

    def down_remote(t, core):
        _, number = half(t, core)
        return remote(OD.at[t % 2], gd_o.at[layer_of(t), number], od_remote_s.at[t % 2], od_r.at[t], at.to_c)

    def out_start(t):
        for one in wide_out(t):
            one.start()
        owner, _ = half(t, c)
        pl.when(owner == c)(lambda: down_local(t).start())
        pl.when(owner != c)(lambda: down_remote(t, c).start())

    def out_wait(t):
        j = t % 2
        pltpu.make_async_copy(OW.at[j], OW.at[j], ow_s.at[j]).wait()
        owner, _ = half(t, c)
        pl.when(owner == c)(lambda: down_local(t).wait())
        pl.when(owner != c)(lambda: down_remote(t, c).wait_send())

    def z_add(t):
        k, j = t % 3, t % 2
        pl.when(t >= 2)(lambda: out_wait(t - 2))
        for one in z_copies(t):
            one.wait()
        for which in range(2):
            g = added(TW[k, which, q, c], ZW[j, which])
            OW[j, which] = g
            wide = g.astype(F32)
            sqw_o[...] += jnp.sum(wide * wide, 0, keepdims=True)
        g = added(TD[k, q, c], ZD[j])
        OD[j] = g
        wide = g.astype(F32)
        sqd_o[...] += jnp.sum(wide * wide, 0, keepdims=True)
        pl.when(t < STEPS - 2)(lambda: credit(z_free, at.to_z))
        out_start(t)

    def between(gate, up, by_mid):
        sig = jax.nn.sigmoid(gate)
        silu = gate * sig
        by_gate = by_mid * up * (sig + silu * (1.0 - sig))
        return (silu * up).astype(BF16), by_gate.astype(BF16), (by_mid * silu).astype(BF16)

    def store_between(m, values):
        for ref, value in zip((MID, DG, DU), values):
            ref[block(m), :] = value

    def layer_one(i):
        gather.whole(i)
        pl.when(i < TILES - 1)(lambda: gather.first(i + 1))

        @pl.when(i == 0)
        def _():
            ACC[...] = jnp.zeros_like(ACC)

        def rows(m, _):
            a = A[block(m), :]
            gate = dot(a, gate_up(WGU, i, 0))
            up = dot(a, gate_up(WGU, i, 1))
            by_mid = dot(DY[block(m), :], down_tile(WD, i), (1, 1)).astype(BF16).astype(F32)
            values = between(gate, up, by_mid)
            store_between(m, values)
            ACC[block(m), :] += dot(values[1], gate_up(WGU, i, 0), (1, 1)) + dot(values[2], gate_up(WGU, i, 1), (1, 1))
            return 0

        lax.fori_loop(0, BLOCKS, rows, 0)

    def kept(n):
        i, m, slot = n // BLOCKS, n % BLOCKS, n % 2
        return [
            pltpu.make_async_copy(
                gu_h.at[i, which, block(m), :], ACC.at[pl.ds(pl.multiple_of(slot * 1024 + which * 512, 512), 512), pl.ds(0, 512)], gus.at[slot, which]
            )
            for which in range(2)
        ]

    def turn():
        a0t_in.start()
        h1_in.wait()
        wd0_in.wait()

        def rows(m, _):
            wide = A[block(m), :].astype(F32)
            by_a = ACC[block(m), :].astype(BF16).astype(F32)
            scale = lax.rsqrt(jnp.mean(wide**2, -1, keepdims=True) + 1e-6)
            along = jnp.mean(by_a * wide, -1, keepdims=True) * scale * scale
            by_h = (scale * (by_a - wide * along)).astype(BF16)
            DY[block(m), :] = added(DY[block(m), :], by_h)
            return 0

        lax.fori_loop(0, BLOCKS, rows, 0)
        for one in kept(0):
            one.start()
        a0t_in.wait()

    def layer_zero(i):
        def rows(m, _):
            n = i * BLOCKS + m
            slot = n % 2

            @pl.when(n + 1 < TILES * BLOCKS)
            def _():
                for one in kept(n + 1):
                    one.start()

            for one in kept(n):
                one.wait()
            gate, up = (ACC[pl.ds(pl.multiple_of(slot * 1024 + which * 512, 512), 512), pl.ds(0, 512)] for which in range(2))
            by_mid = dot(DY[block(m), :], down_tile(WD, i), (1, 1)).astype(BF16).astype(F32)
            store_between(m, between(gate, up, by_mid))
            return 0

        lax.fori_loop(0, BLOCKS, rows, 0)

    def gradients(t):
        k = t % 3

        def rows(half, _):
            for which, by in enumerate((DG, DU)):
                TW[k, which, pl.ds(2 * half, 2)] = dot(AT[half], by[...]).astype(BF16).reshape(2, 2, 112, WIDE)
            return 0

        lax.fori_loop(0, 2, rows, 0)
        TD[k] = dot(MID[...], DY[...], (0, 0)).astype(BF16).reshape(4, 2, 64, D)

    def step(t, _):
        pl.when(t < TILES)(lambda: layer_one(t))
        pl.when(t == TILES)(turn)
        pl.when((t >= TILES) & (t < STEPS))(lambda: layer_zero(t - TILES))

        pl.when(t < TILES - 1)(lambda: gather.second(t + 1))

        @pl.when(t == TILES - 1)
        def _():
            h1_in.start()
            lax.fori_loop(0, TILES, lambda n, _: (down.sent(n), 0)[1], 0)
            wd0_in.start()

        @pl.when((t >= 1) & (t <= STEPS))
        def _():
            pair_add(t - 1)
            first_send(t - 1)

        @pl.when(t >= 2)
        def _():
            second_add(t - 2)
            z_send(t - 2)

        @pl.when(t < STEPS)
        def _():
            gradients(t)
            pair_send(t)

        @pl.when((t >= 1) & (t <= STEPS))
        def _():
            first_add(t - 1)
            second_send(t - 1)

        pl.when(t >= 2)(lambda: z_add(t - 2))
        return 0

    lax.fori_loop(0, STEPS + 2, step, 0)
    out_wait(STEPS - 2)
    out_wait(STEPS - 1)

    lax.fori_loop(0, TILES, lambda n, _: (gather.sent(n), 0)[1], 0)

    def arrived(t, _):
        owner, _ = half(t, 1 - c)
        pl.when(owner == c)(lambda: down_remote(t, 1 - c).wait_recv())
        return 0

    lax.fori_loop(0, STEPS, arrived, 0)


def shape(dims, dtype=BF16):
    return jax.ShapeDtypeStruct(dims, dtype)


def sems(*dims):
    return pltpu.SemaphoreType.DMA(dims)


GATHER_SEMS = [sems(7, TILES)] * 4


def forward(x, w_gate, w_up, w_down):
    return pl.pallas_call(
        forward_kernel,
        name="forward",
        out_shape=[
            shape((TILES, 2, T, WIDE), F32), shape((2, 448, T)), shape((T, D)), shape((T, D)), shape((2, 448, T)), shape((4, 14, 64, D)),
        ],
        in_specs=[ANY] * 4,
        out_specs=[ANY] * 6,
        scratch_shapes=[
            pltpu.VMEM((TILES, 2, 8, 112, WIDE), BF16), pltpu.VMEM((4, 14, 64, D), BF16), pltpu.VMEM((T, D), BF16), pltpu.VMEM((T, D), BF16),
            pltpu.VMEM((2, 448, T), BF16), pltpu.VMEM((TILES, T, WIDE), BF16), pltpu.VMEM((2, 2, ROWS, WIDE), F32),
            pltpu.SemaphoreType.DMA, sems(TILES + 1), sems(2), sems(5), *GATHER_SEMS,
        ],
        compiler_params=pltpu.CompilerParams(collective_id=0, has_side_effects=True, vmem_limit_bytes=VMEM_LIMIT),
    )(x, w_gate, w_up, w_down)


def backward(a1, a1t, h1, dy, a0t, gu, wd0, w_gate, w_up, w_down):
    pair = ((2, 2, 4, 112, WIDE), (2, 4, 64, D))
    two = ((2, 2, 2, 112, WIDE), (2, 2, 64, D))
    one = ((2, 2, 112, WIDE), (2, 64, D))
    return pl.pallas_call(
        backward_kernel,
        name="backward",
        out_shape=[shape((2, 112, FF)), shape((2, 112, FF)), shape((2, 7, 64, D)), shape((1, WIDE), F32), shape((1, D), F32)],
        in_specs=[ANY] * 10,
        out_specs=[ANY] * 3 + [pl.BlockSpec(memory_space=pltpu.VMEM)] * 2,
        scratch_shapes=[
            pltpu.VMEM((TILES, 2, 8, 112, WIDE), BF16), pltpu.VMEM((4, 14, 64, D), BF16), pltpu.VMEM((T, D), BF16), pltpu.VMEM((2, 448, T), BF16),
            pltpu.VMEM((T, D), BF16), pltpu.VMEM((T, D), F32), *[pltpu.VMEM((T, WIDE), BF16)] * 3,
            pltpu.VMEM((3, 2, 4, 2, 112, WIDE), BF16), pltpu.VMEM((3, 4, 2, 64, D), BF16),
            *[pltpu.VMEM(dims, BF16) for dims in (*pair, *two, *one, *one, *one)],
            sems(3), sems(TILES + 1), sems(2, 2), *GATHER_SEMS,
            sems(2, 2), sems(2, 2), sems(6, 2), sems(6, 2), sems(3, 2), sems(3, 2), sems(2, 2), sems(2, 2), sems(2), sems(2), sems(2), sems(STEPS),
            *[pltpu.SemaphoreType.REGULAR] * 6,
        ],
        compiler_params=pltpu.CompilerParams(collective_id=1, has_side_effects=True, vmem_limit_bytes=VMEM_LIMIT),
    )(a1, a1t, h1, dy, a0t, gu, wd0, w_gate, w_up, w_down)


def adamw(w, m, v, g):
    m = 0.9 * m + 0.1 * g
    v = 0.95 * v + 0.05 * g * g
    step = m * lax.rsqrt(v + 1e-8) + 0.1 * w
    return (w - 0.02 * step).astype(BF16), m, v


def solution(mesh):
    def step(x, dy, *arrays):
        weights, m, v = (arrays[i : i + 3] for i in (0, 3, 6))
        shards = (weights[0], weights[1], weights[2].reshape(2, 7, 64, D))
        gu, a0t, h1, a1, a1t, wd0 = forward(x[0], *shards)
        *gradients, squares, squares_down = backward(a1, a1t, h1, dy[0], a0t, gu, wd0, *shards)
        gradients[2] = gradients[2].reshape(2, 448, D)
        squares = lax.psum(jnp.sum(squares) + jnp.sum(squares_down), "s")
        count = lax.psum(1, "s") * sum(g.size for g in gradients)
        factor = jnp.minimum(1.0, 0.5 * lax.rsqrt(squares / count + 1e-30))
        new = [adamw(w.astype(F32), m, v, g.astype(F32) * factor) for w, m, v, g in zip(weights, m, v, gradients, strict=True)]
        return tuple(one[which] for which in range(3) for one in new)

    states, cut = P(("rep", "r", "s"), None, None), P(None, "s", None)
    return jax.shard_map(
        step,
        mesh=mesh,
        in_specs=(states, states) + (cut,) * 9,
        out_specs=(P("rep", "s", None),) * 9,
        check_vma=False,
    )
```

```python
import jax
import jax.numpy as jnp
from jax import lax
from jax.experimental import pallas as pl
from jax.experimental.pallas import tpu as pltpu
from jax.sharding import PartitionSpec as P

MESH = pl.DeviceIdType.MESH
T, D, FF = 2048, 896, 3584
TILES, WIDE, ROWS = 7, 512, 512
BLOCKS = T // ROWS
STEPS = 2 * TILES
SLOTS = 4
F32, BF16 = jnp.float32, jnp.bfloat16
VMEM_LIMIT = 67_043_328
ANY = pl.BlockSpec(memory_space=pl.ANY)


def dot(a, b, contract=(1, 0)):
    return lax.dot_general(a, b, (((contract[0],), (contract[1],)), ((), ())), preferred_element_type=F32)


def normed(h):
    wide = h.astype(F32)
    scale = lax.rsqrt(jnp.mean(wide**2, -1, keepdims=True) + 1e-6)
    return (wide * scale).astype(BF16)


def block(i):
    return pl.ds(pl.multiple_of(i * ROWS, ROWS), ROWS)


def tile_of(j):
    return (j % 2) * 4 + j // 2


class Place:
    def __init__(self):
        r, s = lax.axis_index("r"), lax.axis_index("s")
        c, q = s % 2, s // 2
        y, x = q % 2, q // 2
        self.r, self.s, self.c, self.q = r, s, c, q
        dx, dy = 2 - 4 * x, 1 - 2 * y
        self.qx, self.qy, self.qd = q + dx, q + dy, q + dx + dy
        self.sx, self.sy, self.sc = s + 2 * dx, s + 2 * dy, s + 1 - 2 * c
        self.sd = s + 2 * dx + 2 * dy
        self.sa = self.sx + r * (self.sy - self.sx)
        self.sb = self.sy + r * (self.sx - self.sy)
        self.to_a, self.to_b = {"s": self.sa}, {"s": self.sb}
        self.to_x, self.to_y, self.to_c, self.to_z = {"s": self.sx}, {"s": self.sy}, {"s": self.sc}, {"r": 1 - r}

    def plane(self, n):
        return {"s": (self.s + n) % 8}


def barrier(at):
    sem = pltpu.get_barrier_semaphore()
    partners = [at.plane(n) for n in range(1, 8)] + [at.to_z]
    for to in partners:
        pl.semaphore_signal(sem, inc=1, device_id=to, device_id_type=MESH)
    pl.semaphore_wait(sem, len(partners))


class Gather:
    def __init__(self, at, piece, send, recv):
        self.at, self.piece, self.send, self.recv = at, piece, send, recv

    def copy(self, way, n, shard, to):
        ref = self.piece(n, shard)
        return pltpu.make_async_remote_copy(
            src_ref=ref, dst_ref=ref, send_sem=self.send.at[way, n], recv_sem=self.recv.at[way, n], device_id=to, device_id_type=MESH
        )

    def own(self, n):
        self.copy(0, n, self.at.s, self.at.to_a).start()
        self.copy(3, n, self.at.s, self.at.to_c).start()

    def first(self, n):
        at = self.at
        self.copy(0, n, at.sa, at.to_a).wait_recv()
        self.copy(1, n, at.sa, at.to_z).start()
        self.copy(2, n, at.sa, at.to_b).start()
        self.copy(4, n, at.sa, at.to_c).start()

    def second(self, n):
        at = self.at
        self.copy(1, n, at.sb, at.to_z).wait_recv()
        self.copy(5, n, at.sb, at.to_c).start()
        self.copy(2, n, at.sd, at.to_b).wait_recv()
        self.copy(6, n, at.sd, at.to_c).start()

    def whole(self, n):
        at = self.at
        across = at.sc - at.s
        for way, shard in ((3, at.s), (4, at.sa), (5, at.sb), (6, at.sd)):
            self.copy(way, n, shard + across, at.to_c).wait_recv()

    def sent(self, n):
        at = self.at
        for way, shard, to in (
            (0, at.s, at.to_a), (1, at.sa, at.to_z), (2, at.sa, at.to_b),
            (3, at.s, at.to_c), (4, at.sa, at.to_c), (5, at.sb, at.to_c), (6, at.sd, at.to_c),
        ):
            self.copy(way, n, shard, to).wait_send()


def load_own(at, layer, wg_h, wu_h, wd_h, WGU, WD, own):
    for j in range(TILES):
        for which, w in enumerate((wg_h, wu_h)):
            for k in range(4):
                pltpu.make_async_copy(
                    w.at[layer, :, pl.ds(k * 896 + tile_of(j) * 128, 128)], WGU.at[j, which, at.s, :, pl.ds(k * 128, 128)], own.at[j]
                ).start()
    pltpu.make_async_copy(wd_h.at[layer], WD.at[at.q, pl.ds(at.c * 7, 7)], own.at[TILES]).start()


def wait_own_tile(at, i, WGU, own):
    pltpu.make_async_copy(WGU.at[i, :, at.s], WGU.at[i, :, at.s], own.at[i]).wait()


def wait_own_down(at, wd_h, layer, WD, own):
    pltpu.make_async_copy(wd_h.at[layer], WD.at[at.q, pl.ds(at.c * 7, 7)], own.at[TILES]).wait()


def gathers(at, WGU, WD, sgu, rgu, sd, rd):
    gu = Gather(at, lambda n, s: WGU.at[n, :, s], sgu, rgu)
    down = Gather(at, lambda n, s: WD.at[s // 2, (s % 2) * 7 + n], sd, rd)
    return gu, down


def gate_up(WGU, i, which):
    return WGU[i, which].reshape(D, WIDE)


def down_tile(WD, j):
    return WD[:, pl.ds(2 * tile_of(j), 2)].reshape(WIDE, D)


def forward_kernel(
    x_h, wg_h, wu_h, wd_h,
    gu_o, a0t_o, h1_o, a1_o, a1t_o, wd_o,
    WGU, WD, X, A, AT, MID, ST, ACC,
    load, own, stage, out, sgu, rgu, sd, rd,
):
    at = Place()
    load_own(at, 0, wg_h, wu_h, wd_h, WGU, WD, own)
    x_in = pltpu.make_async_copy(x_h, X, load)
    x_in.start()
    barrier(at)
    gu, down = gathers(at, WGU, WD, sgu, rgu, sd, rd)

    def start_tile(n, _):
        wait_own_tile(at, n, WGU, own)
        gu.own(n)
        return 0

    lax.fori_loop(0, TILES, start_tile, 0)
    wait_own_down(at, wd_h, 0, WD, own)
    lax.fori_loop(0, TILES, lambda n, _: (down.own(n), 0)[1], 0)
    x_in.wait()

    def norm(m, _):
        a = normed(X[block(m), :])
        A[block(m), :] = a
        AT[:, :, block(m)] = a.T.reshape(2, 448, ROWS)
        return 0

    lax.fori_loop(0, BLOCKS, norm, 0)
    a0t_out = pltpu.make_async_copy(AT, a0t_o, out.at[0])
    a0t_out.start()
    gu.first(0)
    gu.first(1)
    gu.second(0)

    def staged(j, m, slot):
        return pltpu.make_async_copy(ST.at[slot], gu_o.at[j, :, block(m), :], stage.at[slot])

    def tile(j, _):
        gu.whole(j)
        pl.when(j < TILES - 2)(lambda: gu.first(j + 2))
        pl.when(j >= TILES - 2)(lambda: down.first(j - TILES + 2))

        def rows(m, _):
            @pl.when(m == 2)
            def _():
                pl.when(j < TILES - 1)(lambda: gu.second(j + 1))
                pl.when(j == TILES - 1)(lambda: down.second(0))

            slot = m % 2
            pl.when(j * BLOCKS + m >= 2)(lambda: staged(j, m, slot).wait())
            a = A[block(m), :]
            gate = dot(a, gate_up(WGU, j, 0))
            up = dot(a, gate_up(WGU, j, 1))
            ST[slot, 0] = gate
            ST[slot, 1] = up
            staged(j, m, slot).start()
            MID[j, block(m), :] = (gate * jax.nn.sigmoid(gate) * up).astype(BF16)
            return 0

        return lax.fori_loop(0, BLOCKS, rows, 0)

    lax.fori_loop(0, TILES, tile, 0)
    down.whole(0)
    down.first(2)
    down.second(1)

    def below(j, _):
        down.whole(j + 1)
        pl.when(j < TILES - 3)(lambda: down.first(j + 3))

        def rows(m, _):
            pl.when((m == 2) & (j < TILES - 2))(lambda: down.second(j + 2))
            part = dot(MID[j, block(m), :], down_tile(WD, j))
            ACC[block(m), :] += part
            return 0

        return lax.fori_loop(0, BLOCKS, rows, 0)

    ACC[...] = jnp.zeros_like(ACC)
    lax.fori_loop(0, TILES - 1, below, 0)
    wd_out = pltpu.make_async_copy(WD, wd_o, out.at[1])
    wd_out.start()
    a0t_out.wait()

    def finish(m, _):
        total = ACC[block(m), :] + dot(MID[TILES - 1, block(m), :], down_tile(WD, TILES - 1))
        h = added(X[block(m), :], total.astype(BF16))
        X[block(m), :] = h
        a = normed(h)
        A[block(m), :] = a
        AT[:, :, block(m)] = a.T.reshape(2, 448, ROWS)
        return 0

    lax.fori_loop(0, BLOCKS, finish, 0)
    outs = [pltpu.make_async_copy(v, o, out.at[2 + k]) for k, (v, o) in enumerate(((X, h1_o), (A, a1_o), (AT, a1t_o)))]
    for o in outs:
        o.start()
    for slot in range(2):
        staged(TILES - 1, slot, slot).wait()

    def sent(n, _):
        gu.sent(n)
        down.sent(n)
        return 0

    lax.fori_loop(0, TILES, sent, 0)
    wd_out.wait()
    for o in outs:
        o.wait()


def added(a, b):
    return (a.astype(F32) + b.astype(F32)).astype(BF16)


def backward_kernel(
    a1_h, a1t_h, h1_h, dy_h, a0t_h, gu_h, wd0_h, wg_h, wu_h, wd_h,
    gg_o, gu_o, gd_o, sq_o,
    WGU, WD, A, AT, DY, ACC, MID, DG, DU, TW, TD, RW, RD, FW, FD, BW, BD, ZW, ZD, OW, OD, SQW, SQD, SQ,
    load, own, gus, sgu, rgu, sd, rd, pair_s, pair_r, first_s, first_r, second_s, second_r, z_s, z_r, ow_s, od_s, od_remote_s, od_r, sq_s, sq_r,
    pair_free, first_x, first_y, second_x, second_y, z_free,
):
    at = Place()
    c, q, qx, qy, qd = at.c, at.q, at.qx, at.qy, at.qd
    load_own(at, 1, wg_h, wu_h, wd_h, WGU, WD, own)
    loads = [pltpu.make_async_copy(h, v, load.at[k]) for k, (h, v) in enumerate(((a1_h, A), (a1t_h, AT), (dy_h, DY)))]
    for one in loads:
        one.start()
    h1_in = pltpu.make_async_copy(h1_h, A, load.at[0])
    wd0_in = pltpu.make_async_copy(wd0_h, WD, load.at[2])
    a0t_in = pltpu.make_async_copy(a0t_h, AT, load.at[1])
    barrier(at)
    gather, down = gathers(at, WGU, WD, sgu, rgu, sd, rd)
    wait_own_down(at, wd_h, 1, WD, own)
    down.own(0)

    def start_tile(j, _):
        pl.when(j < TILES - 1)(lambda: down.own(j + 1))
        wait_own_tile(at, j, WGU, own)
        gather.own(j)
        return 0

    lax.fori_loop(0, TILES, start_tile, 0)
    SQW[...] = jnp.zeros_like(SQW)
    SQD[...] = jnp.zeros_like(SQD)
    ACC[...] = jnp.zeros_like(ACC)
    down.first(0)
    down.first(1)
    down.second(0)
    gather.first(0)
    down.second(1)
    down.whole(0)
    gather.second(0)
    for one in loads:
        one.wait()

    def remote(src, dst, send, recv, to):
        return pltpu.make_async_remote_copy(src_ref=src, dst_ref=dst, send_sem=send, recv_sem=recv, device_id=to, device_id_type=MESH)

    def pair_copy(t, one):
        k, j = t % SLOTS, t % 2
        src, dst = (TW.at[k, one, :, 1 - c], RW.at[j, one]) if one < 2 else (TD.at[k, :, 1 - c], RD.at[j])
        return remote(src, dst, pair_s.at[one, j], pair_r.at[one, j], at.to_c)

    def buffers(t, part):
        k, j = t % SLOTS, t % 2
        if part < 2:
            return (lambda p: TW.at[k, part, p, c]), (lambda n: FW.at[j, part, n]), BW.at[j, part]
        rows = pl.ds(32 * (part - 2), 32)
        return (lambda p: TD.at[k, p, c, rows]), (lambda n: FD.at[j, n, rows]), BD.at[j, rows]

    x, y = (at.to_x, qx), (at.to_y, qy)

    def ways(part):
        return (x, y) if part % 2 == 0 else (y, x)

    def first_copies(t, part):
        mine, into, _ = buffers(t, part)
        to, near = ways(part)[0]
        return [remote(mine(p), into(n), first_s.at[2 * part + n, t % 2], first_r.at[2 * part + n, t % 2], to) for n, p in enumerate((near, qd))]

    def second_copy(t, part):
        mine, _, into = buffers(t, part)
        to, near = ways(part)[1]
        return remote(mine(near), into, second_s.at[part, t % 2], second_r.at[part, t % 2], to)

    def z_copy(t, one):
        k, j = t % SLOTS, t % 2
        src, dst = (TW.at[k, one, q, c], ZW.at[j, one]) if one < 2 else (TD.at[k, q, c], ZD.at[j])
        return remote(src, dst, z_s.at[one, j], z_r.at[one, j], at.to_z)

    def spend(t, *sems):
        @pl.when(t >= 2)
        def _():
            for sem in sems:
                pl.semaphore_wait(sem, 1)

    def free(t, *pairs):
        @pl.when(t < STEPS - 2)
        def _():
            for sem, to in pairs:
                pl.semaphore_signal(sem, inc=1, device_id=to, device_id_type=MESH)

    PARTS = ((0,), (1,), (2, 3))

    def stage_one(t):
        k, j = t % SLOTS, t % 2
        spend(t, first_x, first_y)
        for one in range(3):
            pair_copy(t, one).wait()

            def chip(p, _):
                if one < 2:
                    TW[k, one, p, c] = added(TW[k, one, p, c], RW[j, one, p])
                else:
                    TD[k, p, c] = added(TD[k, p, c], RD[j, p])
                return 0

            lax.fori_loop(0, 4, chip, 0)
            for part in PARTS[one]:
                for copy in first_copies(t, part):
                    copy.start()
        free(t, (pair_free, at.to_c))

    def stage_two(t):
        spend(t, second_x, second_y)
        for part in range(4):
            for copy in first_copies(t, part):
                copy.wait()
            mine, into, _ = buffers(t, part)
            other = ways(part)[1][1]
            mine(other)[...] = added(mine(other)[...], into(1)[...])
            second_copy(t, part).start()
            mine(q)[...] = added(mine(q)[...], into(0)[...])
        free(t, (first_x, at.to_x), (first_y, at.to_y))

    def stage_three(t):
        spend(t, z_free)
        for one in range(3):
            for part in PARTS[one]:
                second_copy(t, part).wait()
                mine, _, into = buffers(t, part)
                mine(q)[...] = added(mine(q)[...], into[...])
            z_copy(t, one).start()
        free(t, (second_x, at.to_x), (second_y, at.to_y))

    def half(t, core):
        number = tile_of(t % TILES) * 2 + core
        return number // 7, number % 7

    def layer_of(t):
        return 1 - t // TILES

    def wide_out(t):
        j, i = t % 2, tile_of(t % TILES)
        for which, o in enumerate((gg_o, gu_o)):
            for k in range(4):
                lanes = pl.ds(pl.multiple_of(k * 896 + i * 128, 128), 128)
                yield pltpu.make_async_copy(OW.at[j, which, :, pl.ds(k * 128, 128)], o.at[layer_of(t), :, lanes], ow_s.at[j])

    def down_local(t):
        _, number = half(t, c)
        return pltpu.make_async_copy(OD.at[t % 2], gd_o.at[layer_of(t), number], od_s.at[t % 2])

    def down_remote(t, core):
        _, number = half(t, core)
        return remote(OD.at[t % 2], gd_o.at[layer_of(t), number], od_remote_s.at[t % 2], od_r.at[t], at.to_c)

    def out_start(t):
        for one in wide_out(t):
            one.start()
        owner, _ = half(t, c)
        pl.when(owner == c)(lambda: down_local(t).start())
        pl.when(owner != c)(lambda: down_remote(t, c).start())

    def out_wait(t):
        j = t % 2
        pltpu.make_async_copy(OW.at[j], OW.at[j], ow_s.at[j]).wait()
        owner, _ = half(t, c)
        pl.when(owner == c)(lambda: down_local(t).wait())
        pl.when(owner != c)(lambda: down_remote(t, c).wait_send())

    def stage_four(t):
        k, j = t % SLOTS, t % 2
        pl.when(t >= 2)(lambda: out_wait(t - 2))
        for one in range(3):
            z_copy(t, one).wait()
            g = added(TW[k, one, q, c], ZW[j, one]) if one < 2 else added(TD[k, q, c], ZD[j])
            wide = g.astype(F32)
            if one < 2:
                OW[j, one] = g
                SQW[...] += jnp.sum((wide * wide).reshape(14, 8, WIDE), 0)
            else:
                OD[j] = g
                SQD[...] += jnp.sum((wide * wide).reshape(8, 8, D), 0)
        free(t, (z_free, at.to_z))
        out_start(t)

    def between(gate, up, by_mid):
        sig = jax.nn.sigmoid(gate)
        silu = gate * sig
        by_gate = by_mid * up * (sig + silu * (1.0 - sig))
        return (silu * up).astype(BF16), by_gate.astype(BF16), (by_mid * silu).astype(BF16)

    def store_between(m, values):
        for ref, value in zip((MID, DG, DU), values):
            ref[block(m), :] = value

    def layer_one(i):
        pl.when(i < TILES - 1)(lambda: down.whole(i + 1))
        gather.whole(i)

        def rows(m, _):
            @pl.when((m == 2) & (i < TILES - 1))
            def _():
                pl.when(i < TILES - 2)(lambda: down.first(i + 2))
                gather.first(i + 1)

            a = A[block(m), :]
            gate = dot(a, gate_up(WGU, i, 0))
            up = dot(a, gate_up(WGU, i, 1))
            by_mid = dot(DY[block(m), :], down_tile(WD, i), (1, 1)).astype(BF16).astype(F32)
            values = between(gate, up, by_mid)
            store_between(m, values)
            ACC[block(m), :] += dot(values[1], gate_up(WGU, i, 0), (1, 1)) + dot(values[2], gate_up(WGU, i, 1), (1, 1))
            return 0

        lax.fori_loop(0, BLOCKS, rows, 0)

    def kept(n):
        i, m, slot = n // BLOCKS, n % BLOCKS, n % 2
        return [
            pltpu.make_async_copy(
                gu_h.at[i, which, block(m), :], ACC.at[pl.ds(pl.multiple_of(slot * 1024 + which * 512, 512), 512), pl.ds(0, 512)], gus.at[slot, which]
            )
            for which in range(2)
        ]

    def turn():
        a0t_in.start()
        h1_in.wait()
        wd0_in.wait()

        def rows(m, _):
            wide = A[block(m), :].astype(F32)
            by_a = ACC[block(m), :].astype(BF16).astype(F32)
            scale = lax.rsqrt(jnp.mean(wide**2, -1, keepdims=True) + 1e-6)
            along = jnp.mean(by_a * wide, -1, keepdims=True) * scale * scale
            by_h = (scale * (by_a - wide * along)).astype(BF16)
            DY[block(m), :] = added(DY[block(m), :], by_h)
            return 0

        lax.fori_loop(0, BLOCKS, rows, 0)
        for one in kept(0):
            one.start()
        a0t_in.wait()

    def layer_zero(i):
        def rows(m, _):
            n = i * BLOCKS + m
            slot = n % 2

            @pl.when(n + 1 < TILES * BLOCKS)
            def _():
                for one in kept(n + 1):
                    one.start()

            for one in kept(n):
                one.wait()
            gate, up = (ACC[pl.ds(pl.multiple_of(slot * 1024 + which * 512, 512), 512), pl.ds(0, 512)] for which in range(2))
            by_mid = dot(DY[block(m), :], down_tile(WD, i), (1, 1)).astype(BF16).astype(F32)
            store_between(m, between(gate, up, by_mid))
            return 0

        lax.fori_loop(0, BLOCKS, rows, 0)

    def gradients(t):
        k = t % SLOTS
        spend(t, pair_free)
        for which, by in enumerate((DG, DU)):

            def rows(half, _):
                TW[k, which, pl.ds(2 * half, 2)] = dot(AT[half], by[...]).astype(BF16).reshape(2, 2, 112, WIDE)
                return 0

            lax.fori_loop(0, 2, rows, 0)
            pair_copy(t, which).start()
        TD[k] = dot(MID[...], DY[...], (0, 0)).astype(BF16).reshape(4, 2, 64, D)
        pair_copy(t, 2).start()

    def step(t, _):
        pl.when(t < TILES)(lambda: layer_one(t))
        pl.when(t == TILES)(turn)
        pl.when((t >= TILES) & (t < STEPS))(lambda: layer_zero(t - TILES))
        pl.when((t >= 1) & (t <= STEPS))(lambda: stage_one(t - 1))
        pl.when((t >= 2) & (t <= STEPS + 1))(lambda: stage_two(t - 2))
        pl.when((t >= 3) & (t <= STEPS + 2))(lambda: stage_three(t - 3))
        pl.when(t >= 4)(lambda: stage_four(t - 4))

        @pl.when(t < TILES - 1)
        def _():
            pl.when(t < TILES - 2)(lambda: down.second(t + 2))
            gather.second(t + 1)

        @pl.when(t == TILES - 1)
        def _():
            h1_in.start()
            lax.fori_loop(0, TILES, lambda n, _: (down.sent(n), 0)[1], 0)
            wd0_in.start()

        pl.when(t < STEPS)(lambda: gradients(t))
        return 0

    lax.fori_loop(0, STEPS + 4, step, 0)

    mine = jnp.sum(SQW[...], keepdims=True) + jnp.sum(SQD[...], keepdims=True)
    SQ[at.s] = jnp.broadcast_to(mine, (8, 128))

    def square(n, from_):
        return remote(SQ.at[from_], SQ.at[from_], sq_s.at[n - 1], sq_r.at[n - 1], at.plane(n))

    for n in range(1, 8):
        square(n, at.s).start()
    out_wait(STEPS - 2)
    out_wait(STEPS - 1)

    lax.fori_loop(0, TILES, lambda n, _: (gather.sent(n), 0)[1], 0)

    def arrived(t, _):
        owner, _ = half(t, 1 - c)
        pl.when(owner == c)(lambda: down_remote(t, 1 - c).wait_recv())
        return 0

    lax.fori_loop(0, STEPS, arrived, 0)
    for n in range(1, 8):
        square(n, (at.s + 8 - n) % 8).wait_recv()
        square(n, at.s).wait_send()
    total = SQ[0]
    for n in range(1, 8):
        total += SQ[n]
    sq_o[...] = total


def shape(dims, dtype=BF16):
    return jax.ShapeDtypeStruct(dims, dtype)


def sems(*dims):
    return pltpu.SemaphoreType.DMA(dims)


GATHER_SEMS = [sems(7, TILES)] * 4


def forward(x, w_gate, w_up, w_down):
    return pl.pallas_call(
        forward_kernel,
        name="forward",
        out_shape=[
            shape((TILES, 2, T, WIDE), F32), shape((2, 448, T)), shape((T, D)), shape((T, D)), shape((2, 448, T)), shape((4, 14, 64, D)),
        ],
        in_specs=[ANY] * 4,
        out_specs=[ANY] * 6,
        scratch_shapes=[
            pltpu.VMEM((TILES, 2, 8, 112, WIDE), BF16), pltpu.VMEM((4, 14, 64, D), BF16), pltpu.VMEM((T, D), BF16), pltpu.VMEM((T, D), BF16),
            pltpu.VMEM((2, 448, T), BF16), pltpu.VMEM((TILES, T, WIDE), BF16), pltpu.VMEM((2, 2, ROWS, WIDE), F32), pltpu.VMEM((T, D), F32),
            pltpu.SemaphoreType.DMA, sems(TILES + 1), sems(2), sems(5), *GATHER_SEMS,
        ],
        compiler_params=pltpu.CompilerParams(collective_id=0, has_side_effects=True, vmem_limit_bytes=VMEM_LIMIT),
    )(x, w_gate, w_up, w_down)


def backward(a1, a1t, h1, dy, a0t, gu, wd0, w_gate, w_up, w_down):
    pair = ((2, 2, 4, 112, WIDE), (2, 4, 64, D))
    two = ((2, 2, 2, 112, WIDE), (2, 2, 64, D))
    one = ((2, 2, 112, WIDE), (2, 64, D))
    return pl.pallas_call(
        backward_kernel,
        name="backward",
        out_shape=[shape((2, 112, FF)), shape((2, 112, FF)), shape((2, 7, 64, D)), shape((8, 128), F32)],
        in_specs=[ANY] * 10,
        out_specs=[ANY] * 3 + [pl.BlockSpec(memory_space=pltpu.VMEM)],
        scratch_shapes=[
            pltpu.VMEM((TILES, 2, 8, 112, WIDE), BF16), pltpu.VMEM((4, 14, 64, D), BF16), pltpu.VMEM((T, D), BF16), pltpu.VMEM((2, 448, T), BF16),
            pltpu.VMEM((T, D), BF16), pltpu.VMEM((T, D), F32), *[pltpu.VMEM((T, WIDE), BF16)] * 3,
            pltpu.VMEM((SLOTS, 2, 4, 2, 112, WIDE), BF16), pltpu.VMEM((SLOTS, 4, 2, 64, D), BF16),
            *[pltpu.VMEM(dims, BF16) for dims in (*pair, *two, *one, *one, *one)],
            pltpu.VMEM((8, WIDE), F32), pltpu.VMEM((8, D), F32), pltpu.VMEM((8, 8, 128), F32),
            sems(3), sems(TILES + 1), sems(2, 2), *GATHER_SEMS,
            sems(3, 2), sems(3, 2), sems(8, 2), sems(8, 2), sems(4, 2), sems(4, 2), sems(3, 2), sems(3, 2), sems(2), sems(2), sems(2), sems(STEPS),
            sems(7), sems(7),
            *[pltpu.SemaphoreType.REGULAR] * 6,
        ],
        compiler_params=pltpu.CompilerParams(collective_id=1, has_side_effects=True, vmem_limit_bytes=VMEM_LIMIT),
    )(a1, a1t, h1, dy, a0t, gu, wd0, w_gate, w_up, w_down)


def adamw(w, m, v, g):
    m = 0.9 * m + 0.1 * g
    v = 0.95 * v + 0.05 * g * g
    step = m * lax.rsqrt(v + 1e-8) + 0.1 * w
    return (w - 0.02 * step).astype(BF16), m, v


def solution(mesh):
    def step(x, dy, *arrays):
        weights, m, v = (arrays[i : i + 3] for i in (0, 3, 6))
        shards = (weights[0], weights[1], weights[2].reshape(2, 7, 64, D))
        gu, a0t, h1, a1, a1t, wd0 = forward(x[0], *shards)
        *gradients, squares = backward(a1, a1t, h1, dy[0], a0t, gu, wd0, *shards)
        gradients[2] = gradients[2].reshape(2, 448, D)
        count = mesh.shape["s"] * sum(g.size for g in gradients)
        factor = jnp.minimum(1.0, 0.5 * lax.rsqrt(squares[0, 0] / count + 1e-30))
        new = [adamw(w.astype(F32), m, v, g.astype(F32) * factor) for w, m, v, g in zip(weights, m, v, gradients, strict=True)]
        return tuple(one[which] for which in range(3) for one in new)

    states, cut = P(("rep", "r", "s"), None, None), P(None, "s", None)
    return jax.shard_map(
        step,
        mesh=mesh,
        in_specs=(states, states) + (cut,) * 9,
        out_specs=(P("rep", "s", None),) * 9,
        check_vma=False,
    )
```

```python
import jax
import jax.numpy as jnp
from jax import lax
from jax.experimental import pallas as pl
from jax.experimental.pallas import tpu as pltpu
from jax.sharding import PartitionSpec as P

MESH = pl.DeviceIdType.MESH
T, D, FF = 2048, 896, 3584
TILES, WIDE, ROWS = 7, 512, 512
BLOCKS = T // ROWS
STEPS = 2 * TILES
AHEAD = 2
SLOTS = 4
F32, BF16 = jnp.float32, jnp.bfloat16
VMEM_LIMIT = 67_043_328
ANY = pl.BlockSpec(memory_space=pl.ANY)


def dot(a, b, contract=(1, 0)):
    return lax.dot_general(a, b, (((contract[0],), (contract[1],)), ((), ())), preferred_element_type=F32)


def loop(n, body):
    def run(i, carry):
        body(i)
        return carry

    lax.fori_loop(0, n, run, 0)


def normed(h):
    wide = h.astype(F32)
    scale = lax.rsqrt(jnp.mean(wide**2, -1, keepdims=True) + 1e-6)
    return (wide * scale).astype(BF16)


def block(i):
    return pl.ds(pl.multiple_of(i * ROWS, ROWS), ROWS)


def tile_of(j):
    return (j % 2) * 4 + j // 2


class Place:
    def __init__(self):
        r, s = lax.axis_index("r"), lax.axis_index("s")
        c, q = s % 2, s // 2
        y, x = q % 2, q // 2
        self.r, self.s, self.c, self.q = r, s, c, q
        dx, dy = 2 - 4 * x, 1 - 2 * y
        self.qx, self.qy, self.qd = q + dx, q + dy, q + dx + dy
        self.sx, self.sy, self.sc = s + 2 * dx, s + 2 * dy, s + 1 - 2 * c
        self.sd = s + 2 * dx + 2 * dy
        self.sa = self.sx + r * (self.sy - self.sx)
        self.sb = self.sy + r * (self.sx - self.sy)
        self.to_a, self.to_b = {"s": self.sa}, {"s": self.sb}
        self.to_x, self.to_y, self.to_c, self.to_z = {"s": self.sx}, {"s": self.sy}, {"s": self.sc}, {"r": 1 - r}

    def plane(self, n):
        return {"s": (self.s + n) % 8}


def barrier(at):
    sem = pltpu.get_barrier_semaphore()
    partners = [at.plane(n) for n in range(1, 8)] + [at.to_z]
    for to in partners:
        pl.semaphore_signal(sem, inc=1, device_id=to, device_id_type=MESH)
    pl.semaphore_wait(sem, len(partners))


class Gather:
    def __init__(self, at, piece, send, recv):
        self.at, self.piece, self.send, self.recv = at, piece, send, recv

    def copy(self, way, n, shard, to):
        ref = self.piece(n, shard)
        return pltpu.make_async_remote_copy(
            src_ref=ref, dst_ref=ref, send_sem=self.send.at[way, n], recv_sem=self.recv.at[way, n], device_id=to, device_id_type=MESH
        )

    def own(self, n):
        self.copy(0, n, self.at.s, self.at.to_a).start()
        self.copy(3, n, self.at.s, self.at.to_c).start()

    def first(self, n):
        at = self.at
        self.copy(0, n, at.sa, at.to_a).wait_recv()
        self.copy(1, n, at.sa, at.to_z).start()
        self.copy(2, n, at.sa, at.to_b).start()
        self.copy(4, n, at.sa, at.to_c).start()

    def second(self, n):
        at = self.at
        self.copy(1, n, at.sb, at.to_z).wait_recv()
        self.copy(5, n, at.sb, at.to_c).start()
        self.copy(2, n, at.sd, at.to_b).wait_recv()
        self.copy(6, n, at.sd, at.to_c).start()

    def whole(self, n):
        at = self.at
        across = at.sc - at.s
        for way, shard in ((3, at.s), (4, at.sa), (5, at.sb), (6, at.sd)):
            self.copy(way, n, shard + across, at.to_c).wait_recv()

    def sent(self, n):
        at = self.at
        for way, shard, to in (
            (0, at.s, at.to_a), (1, at.sa, at.to_z), (2, at.sa, at.to_b),
            (3, at.s, at.to_c), (4, at.sa, at.to_c), (5, at.sb, at.to_c), (6, at.sd, at.to_c),
        ):
            self.copy(way, n, shard, to).wait_send()


def load_tile(at, layer, j, wg_h, wu_h, into, sem):
    for which, w in enumerate((wg_h, wu_h)):
        for k in range(4):
            pltpu.make_async_copy(w.at[layer, :, pl.ds(k * 896 + tile_of(j) * 128, 128)], into.at[which, at.s, :, pl.ds(k * 128, 128)], sem).start()


def own_down(at, layer, wd_h, WD, own):
    skip = layer * AHEAD
    return pltpu.make_async_copy(wd_h.at[layer, pl.ds(skip, 7 - skip)], WD.at[at.q, pl.ds(at.c * 7 + skip, 7 - skip)], own.at[TILES])


def wait_own_tile(at, i, WGU, own):
    pltpu.make_async_copy(WGU.at[i, :, at.s], WGU.at[i, :, at.s], own.at[i]).wait()


def gathers(at, WGU, WD, sgu, rgu, sd, rd):
    gu = Gather(at, lambda n, s: WGU.at[n, :, s], sgu, rgu)
    down = Gather(at, lambda n, s: WD.at[s // 2, (s % 2) * 7 + n], sd, rd)
    return gu, down


def gate_up(WGU, i, which):
    return WGU[i, which].reshape(D, WIDE)


def down_tile(WD, j):
    return WD[:, pl.ds(2 * tile_of(j), 2)].reshape(WIDE, D)


def forward_kernel(
    x_h, wg_h, wu_h, wd_h,
    gu_o, a0t_o, h1_o, a1_o, a1t_o, wd_o, wgu1_o, wd1_o,
    WGU, WD, X, A, AT, MID, ST, ACC, WGU1, WD1,
    load, own, stage, out, done, sgu, rgu, sd, rd, own1, sgu1, rgu1, sd1, rd1,
):
    at = Place()
    for j in range(TILES):
        load_tile(at, 0, j, wg_h, wu_h, WGU.at[j], own.at[j])
    own_down(at, 0, wd_h, WD, own).start()
    load_tile(at, 1, 0, wg_h, wu_h, WGU1.at[0], own1.at[0])
    down1_in = pltpu.make_async_copy(wd_h.at[1, pl.ds(0, AHEAD)], WD1.at[at.q, at.c], own1.at[1])
    down1_in.start()
    x_in = pltpu.make_async_copy(x_h, X, load)
    x_in.start()
    barrier(at)
    gu, down = gathers(at, WGU, WD, sgu, rgu, sd, rd)
    gu1 = Gather(at, lambda n, s: WGU1.at[n, :, s], sgu1, rgu1)
    down1 = Gather(at, lambda n, s: WD1.at[s // 2, s % 2, n], sd1, rd1)

    def start_tile(n):
        wait_own_tile(at, n, WGU, own)
        gu.own(n)

    loop(TILES, start_tile)
    own_down(at, 0, wd_h, WD, own).wait()
    loop(TILES, lambda n: down.own(n))
    down1_in.wait()
    loop(AHEAD, lambda n: down1.own(n))
    wait_own_tile(at, 0, WGU1, own1)
    gu1.own(0)
    x_in.wait()

    def norm(m):
        a = normed(X[block(m), :])
        A[block(m), :] = a
        AT[:, :, block(m)] = a.T.reshape(2, 448, ROWS)

    loop(BLOCKS, norm)
    a0t_out = pltpu.make_async_copy(AT, a0t_o, out.at[0])
    a0t_out.start()
    gu.first(0)
    gu.first(1)
    gu.second(0)

    def staged(j, m, slot):
        return pltpu.make_async_copy(ST.at[slot], gu_o.at[j, :, block(m), :], stage.at[slot])

    def tile(j):
        gu.whole(j)

        def rows(m):
            @pl.when(m == 1)
            def _():
                pl.when(j < TILES - 2)(lambda: gu.first(j + 2))
                pl.when(j >= TILES - 2)(lambda: down.first(j - TILES + 2))

            @pl.when(m == 3)
            def _():
                pl.when(j < TILES - 1)(lambda: gu.second(j + 1))
                pl.when(j == TILES - 1)(lambda: down.second(0))

            slot = m % 2
            pl.when(j * BLOCKS + m >= 2)(lambda: staged(j, m, slot).wait())
            a = A[block(m), :]
            gate = dot(a, gate_up(WGU, j, 0))
            up = dot(a, gate_up(WGU, j, 1))
            ST[slot, 0] = gate
            ST[slot, 1] = up
            staged(j, m, slot).start()
            MID[j, block(m), :] = (gate * jax.nn.sigmoid(gate) * up).astype(BF16)

        loop(BLOCKS, rows)

    loop(TILES, tile)
    down.whole(0)
    down.first(2)
    down.second(1)

    def below(j):
        down.whole(j + 1)
        pl.when(j < TILES - 3)(lambda: down.first(j + 3))

        def rows(m):
            pl.when((m == 2) & (j < TILES - 2))(lambda: down.second(j + 2))

            @pl.when((m == 2) & (j >= TILES - 3))
            def _():
                pl.when(j == TILES - 3)(lambda: down1.first(0))
                pl.when(j == TILES - 2)(lambda: down1.first(1))

            part = dot(MID[j, block(m), :], down_tile(WD, j))
            ACC[block(m), :] += part

        loop(BLOCKS, rows)

    ACC[...] = jnp.zeros_like(ACC)
    loop(TILES - 1, below)
    wd_out = pltpu.make_async_copy(WD, wd_o, out.at[1])
    wd_out.start()
    a0t_out.wait()

    gu1.first(0)
    down1.second(0)

    def finish(m):
        @pl.when(m == 2)
        def _():
            down1.second(1)
            gu1.second(0)

        total = ACC[block(m), :] + dot(MID[TILES - 1, block(m), :], down_tile(WD, TILES - 1))
        h = added(X[block(m), :], total.astype(BF16))
        X[block(m), :] = h
        a = normed(h)
        A[block(m), :] = a
        AT[:, :, block(m)] = a.T.reshape(2, 448, ROWS)
        for one in block_out(m):
            one.start()

    def block_out(m):
        return [
            pltpu.make_async_copy(X.at[block(m), :], h1_o.at[block(m), :], done.at[0, m]),
            pltpu.make_async_copy(A.at[block(m), :], a1_o.at[block(m), :], done.at[1, m]),
            pltpu.make_async_copy(AT.at[:, :, block(m)], a1t_o.at[:, :, block(m)], done.at[2, m]),
        ]

    loop(BLOCKS, finish)
    gu1.whole(0)
    loop(AHEAD, lambda n: down1.whole(n))
    pairs = ((WGU1, wgu1_o), (WD1, wd1_o))
    outs = [pltpu.make_async_copy(v, o, out.at[2 + k]) for k, (v, o) in enumerate(pairs)]
    for o in outs:
        o.start()
    for slot in range(2):
        staged(TILES - 1, slot, slot).wait()

    def sent(n):
        gu.sent(n)
        down.sent(n)

    loop(TILES, sent)
    gu1.sent(0)
    loop(AHEAD, lambda n: down1.sent(n))
    wd_out.wait()

    def blocks_left(m):
        for one in block_out(m):
            one.wait()

    loop(BLOCKS, blocks_left)
    for o in outs:
        o.wait()


def added(a, b):
    return (a.astype(F32) + b.astype(F32)).astype(BF16)


def backward_kernel(
    a1_h, a1t_h, h1_h, dy_h, a0t_h, gu_h, wd0_h, wgu1_h, wd1_h, wg_h, wu_h, wd_h,
    gg_o, gu_o, gd_o, sq_o,
    WGU, WD, A, AT, DY, ACC, MID, DG, DU, TW, TD, RW, RD, FW, FD, BW, BD, ZW, ZD, OW, OD, SQW, SQD, SQ,
    load, own, gus, sgu, rgu, sd, rd, pair_s, pair_r, first_s, first_r, second_s, second_r, z_s, z_r, ow_s, od_s, od_remote_s, od_r, sq_s, sq_r,
    pair_free, first_x, first_y, second_x, second_y, z_free,
):
    at = Place()
    c, q, qx, qy, qd = at.c, at.q, at.qx, at.qy, at.qd
    own_down(at, 1, wd_h, WD, own).start()
    for j in range(1, TILES):
        load_tile(at, 1, j, wg_h, wu_h, WGU.at[j], own.at[j])
    pairs = [(a1_h, A), (wgu1_h.at[0], WGU.at[0]), (dy_h, DY), (a1t_h, AT)]
    pairs += [(wd1_h.at[:, core], WD.at[:, pl.ds(7 * core, AHEAD)]) for core in range(2)]
    loads = [pltpu.make_async_copy(h, v, load.at[k]) for k, (h, v) in enumerate(pairs)]
    for one in loads:
        one.start()
    h1_in = pltpu.make_async_copy(h1_h, A, load.at[0])
    wd0_in = pltpu.make_async_copy(wd0_h, WD, load.at[2])
    a0t_in = pltpu.make_async_copy(a0t_h, AT, load.at[1])
    barrier(at)
    gather, down = gathers(at, WGU, WD, sgu, rgu, sd, rd)
    own_down(at, 1, wd_h, WD, own).wait()

    def start_tile(j):
        down.own(j + 2)
        wait_own_tile(at, j + 1, WGU, own)
        gather.own(j + 1)

    loop(TILES - AHEAD, start_tile)
    wait_own_tile(at, TILES - 1, WGU, own)
    gather.own(TILES - 1)
    SQW[...] = jnp.zeros_like(SQW)
    SQD[...] = jnp.zeros_like(SQD)
    ACC[...] = jnp.zeros_like(ACC)
    for one in loads:
        one.wait()

    def remote(src, dst, send, recv, to):
        return pltpu.make_async_remote_copy(src_ref=src, dst_ref=dst, send_sem=send, recv_sem=recv, device_id=to, device_id_type=MESH)

    def pair_copy(t, one):
        k, j = t % SLOTS, t % 2
        src, dst = (TW.at[k, one, :, 1 - c], RW.at[j, one]) if one < 2 else (TD.at[k, :, 1 - c], RD.at[j])
        return remote(src, dst, pair_s.at[one, j], pair_r.at[one, j], at.to_c)

    def buffers(t, part):
        k, j = t % SLOTS, t % 2
        if part < 2:
            return (lambda p: TW.at[k, part, p, c]), (lambda n: FW.at[j, part, n]), BW.at[j, part]
        rows = pl.ds(32 * (part - 2), 32)
        return (lambda p: TD.at[k, p, c, rows]), (lambda n: FD.at[j, n, rows]), BD.at[j, rows]

    x, y = (at.to_x, qx), (at.to_y, qy)

    def ways(part):
        return (x, y) if part % 2 == 0 else (y, x)

    def first_copies(t, part):
        mine, into, _ = buffers(t, part)
        (to, near), _ = ways(part)
        return [remote(mine(p), into(n), first_s.at[2 * part + n, t % 2], first_r.at[2 * part + n, t % 2], to) for n, p in enumerate((near, qd))]

    def second_copy(t, part):
        mine, _, into = buffers(t, part)
        _, (to, near) = ways(part)
        return remote(mine(near), into, second_s.at[part, t % 2], second_r.at[part, t % 2], to)

    def z_copy(t, one):
        k, j = t % SLOTS, t % 2
        src, dst = (TW.at[k, one, q, c], ZW.at[j, one]) if one < 2 else (TD.at[k, q, c], ZD.at[j])
        return remote(src, dst, z_s.at[one, j], z_r.at[one, j], at.to_z)

    def spend(t, *sems):
        @pl.when(t >= 2)
        def _():
            for sem in sems:
                pl.semaphore_wait(sem, 1)

    def free(t, *pairs):
        @pl.when(t < STEPS - 2)
        def _():
            for sem, to in pairs:
                pl.semaphore_signal(sem, inc=1, device_id=to, device_id_type=MESH)

    PARTS = ((0,), (1,), (2, 3))

    def stage_one(t, one):
        k, j = t % SLOTS, t % 2
        pair_copy(t, one).wait()

        def chip(p):
            if one < 2:
                TW[k, one, p, c] = added(TW[k, one, p, c], RW[j, one, p])
            else:
                TD[k, p, c] = added(TD[k, p, c], RD[j, p])

        loop(4, chip)
        for part in PARTS[one]:
            for copy in first_copies(t, part):
                copy.start()

    def stage_two(t):
        spend(t, second_x, second_y)
        for part in range(4):
            for copy in first_copies(t, part):
                copy.wait()
            mine, into, _ = buffers(t, part)
            _, (_, other) = ways(part)
            mine(other)[...] = added(mine(other)[...], into(1)[...])
            second_copy(t, part).start()
            mine(q)[...] = added(mine(q)[...], into(0)[...])
        free(t, (first_x, at.to_x), (first_y, at.to_y))

    def stage_three(t):
        spend(t, z_free)
        for one in range(3):
            for part in PARTS[one]:
                second_copy(t, part).wait()
                mine, _, into = buffers(t, part)
                mine(q)[...] = added(mine(q)[...], into[...])
            z_copy(t, one).start()
        free(t, (second_x, at.to_x), (second_y, at.to_y))

    def half(t, core):
        number = tile_of(t % TILES) * 2 + core
        return number // 7, pl.ds(pl.multiple_of(number % 7 * 64, 64), 64)

    def layer_of(t):
        return 1 - t // TILES

    def wide_out(t):
        j, i = t % 2, tile_of(t % TILES)
        for which, o in enumerate((gg_o, gu_o)):
            for k in range(4):
                lanes = pl.ds(pl.multiple_of(k * 896 + i * 128, 128), 128)
                yield pltpu.make_async_copy(OW.at[j, which, :, pl.ds(k * 128, 128)], o.at[layer_of(t), :, lanes], ow_s.at[j])

    def down_local(t):
        _, number = half(t, c)
        return pltpu.make_async_copy(OD.at[t % 2], gd_o.at[layer_of(t), number], od_s.at[t % 2])

    def down_remote(t, core):
        _, number = half(t, core)
        return remote(OD.at[t % 2], gd_o.at[layer_of(t), number], od_remote_s.at[t % 2], od_r.at[t], at.to_c)

    def out_start(t):
        for one in wide_out(t):
            one.start()
        owner, _ = half(t, c)
        pl.when(owner == c)(lambda: down_local(t).start())
        pl.when(owner != c)(lambda: down_remote(t, c).start())

    def out_wait(t):
        j = t % 2
        pltpu.make_async_copy(OW.at[j], OW.at[j], ow_s.at[j]).wait()
        owner, _ = half(t, c)
        pl.when(owner == c)(lambda: down_local(t).wait())
        pl.when(owner != c)(lambda: down_remote(t, c).wait_send())

    def stage_four(t):
        k, j = t % SLOTS, t % 2
        pl.when(t >= 2)(lambda: out_wait(t - 2))
        for one in range(3):
            z_copy(t, one).wait()
            g = added(TW[k, one, q, c], ZW[j, one]) if one < 2 else added(TD[k, q, c], ZD[j])
            wide = g.astype(F32)
            if one < 2:
                OW[j, one] = g
                SQW[...] += jnp.sum((wide * wide).reshape(14, 8, WIDE), 0)
            else:
                OD[j] = g
                SQD[...] += jnp.sum((wide * wide).reshape(8, 8, D), 0)
        free(t, (z_free, at.to_z))
        out_start(t)

    def between(gate, up, by_mid):
        sig = jax.nn.sigmoid(gate)
        silu = gate * sig
        by_gate = by_mid * up * (sig + silu * (1.0 - sig))
        return (silu * up).astype(BF16), by_gate.astype(BF16), (by_mid * silu).astype(BF16)

    def store_between(m, values):
        for ref, value in zip((MID, DG, DU), values):
            ref[block(m), :] = value

    def layer_one(i):
        pl.when((i > 0) & (i < TILES - 1))(lambda: down.whole(i + 1))
        pl.when(i > 0)(lambda: gather.whole(i))

        def rows(m):
            @pl.when((m == 2) & (i < TILES - 1))
            def _():
                pl.when(i < TILES - 2)(lambda: down.first(i + 2))
                gather.first(i + 1)

            a = A[block(m), :]
            gate = dot(a, gate_up(WGU, i, 0))
            up = dot(a, gate_up(WGU, i, 1))
            by_mid = dot(DY[block(m), :], down_tile(WD, i), (1, 1)).astype(BF16).astype(F32)
            values = between(gate, up, by_mid)
            store_between(m, values)
            ACC[block(m), :] += dot(values[1], gate_up(WGU, i, 0), (1, 1)) + dot(values[2], gate_up(WGU, i, 1), (1, 1))

        loop(BLOCKS, rows)

    def kept(n):
        i, m, slot = n // BLOCKS, n % BLOCKS, n % 2
        return [
            pltpu.make_async_copy(
                gu_h.at[i, which, block(m), :], ACC.at[pl.ds(pl.multiple_of(slot * 1024 + which * 512, 512), 512), pl.ds(0, 512)], gus.at[slot, which]
            )
            for which in range(2)
        ]

    def turn():
        a0t_in.start()
        h1_in.wait()
        wd0_in.wait()

        def rows(m):
            wide = A[block(m), :].astype(F32)
            by_a = ACC[block(m), :].astype(BF16).astype(F32)
            scale = lax.rsqrt(jnp.mean(wide**2, -1, keepdims=True) + 1e-6)
            along = jnp.mean(by_a * wide, -1, keepdims=True) * scale * scale
            by_h = (scale * (by_a - wide * along)).astype(BF16)
            DY[block(m), :] = added(DY[block(m), :], by_h)

        loop(BLOCKS, rows)
        for one in kept(0):
            one.start()
        a0t_in.wait()

    def layer_zero(i):
        def rows(m):
            n = i * BLOCKS + m
            slot = n % 2

            @pl.when(n + 1 < TILES * BLOCKS)
            def _():
                for one in kept(n + 1):
                    one.start()

            for one in kept(n):
                one.wait()
            gate, up = (ACC[pl.ds(pl.multiple_of(slot * 1024 + which * 512, 512), 512), pl.ds(0, 512)] for which in range(2))
            by_mid = dot(DY[block(m), :], down_tile(WD, i), (1, 1)).astype(BF16).astype(F32)
            store_between(m, between(gate, up, by_mid))

        loop(BLOCKS, rows)

    def gradients(t):
        k = t % SLOTS
        spend(t, pair_free)
        for which, by in enumerate((DG, DU)):

            def rows(half):
                TW[k, which, pl.ds(2 * half, 2)] = dot(AT[half], by[...]).astype(BF16).reshape(2, 2, 112, WIDE)

            loop(2, rows)
            pair_copy(t, which).start()
        TD[k] = dot(MID[...], DY[...], (0, 0)).astype(BF16).reshape(4, 2, 64, D)
        pair_copy(t, 2).start()

    def step(t):
        pl.when(t < TILES)(lambda: layer_one(t))
        pl.when(t == TILES)(turn)
        pl.when((t >= TILES) & (t < STEPS))(lambda: layer_zero(t - TILES))

        @pl.when((t >= 1) & (t <= STEPS))
        def _():
            spend(t - 1, first_x, first_y)
            for one in range(3):
                stage_one(t - 1, one)
            free(t - 1, (pair_free, at.to_c))

        pl.when((t >= 3) & (t <= STEPS + 2))(lambda: stage_three(t - 3))
        pl.when((t >= 2) & (t <= STEPS + 1))(lambda: stage_two(t - 2))
        pl.when(t >= 4)(lambda: stage_four(t - 4))

        @pl.when(t < TILES - 1)
        def _():
            pl.when(t < TILES - 2)(lambda: down.second(t + 2))
            gather.second(t + 1)

        @pl.when(t == TILES - 1)
        def _():
            h1_in.start()
            loop(TILES - AHEAD, lambda n: down.sent(n + AHEAD))
            wd0_in.start()

        pl.when(t < STEPS)(lambda: gradients(t))

    loop(STEPS + 4, step)

    mine = jnp.sum(SQW[...], keepdims=True) + jnp.sum(SQD[...], keepdims=True)
    SQ[at.s] = jnp.broadcast_to(mine, (8, 128))

    def square(n, from_):
        return remote(SQ.at[from_], SQ.at[from_], sq_s.at[n - 1], sq_r.at[n - 1], at.plane(n))

    for n in range(1, 8):
        square(n, at.s).start()
    out_wait(STEPS - 2)
    out_wait(STEPS - 1)

    loop(TILES - 1, lambda n: gather.sent(n + 1))

    def arrived(t):
        owner, _ = half(t, 1 - c)
        pl.when(owner == c)(lambda: down_remote(t, 1 - c).wait_recv())

    loop(STEPS, arrived)
    for n in range(1, 8):
        square(n, (at.s + 8 - n) % 8).wait_recv()
        square(n, at.s).wait_send()
    total = SQ[0]
    for n in range(1, 8):
        total += SQ[n]
    sq_o[...] = total


def shape(dims, dtype=BF16):
    return jax.ShapeDtypeStruct(dims, dtype)


def sems(*dims):
    return pltpu.SemaphoreType.DMA(dims)


GATHER_SEMS = [sems(7, TILES)] * 4


def forward(x, w_gate, w_up, w_down):
    return pl.pallas_call(
        forward_kernel,
        name="forward",
        out_shape=[
            shape((TILES, 2, T, WIDE), F32), shape((2, 448, T)), shape((T, D)), shape((T, D)), shape((2, 448, T)), shape((4, 14, 64, D)),
            shape((1, 2, 8, 112, WIDE)), shape((4, 2, AHEAD, 64, D)),
        ],
        in_specs=[ANY] * 4,
        out_specs=[ANY] * 8,
        scratch_shapes=[
            pltpu.VMEM((TILES, 2, 8, 112, WIDE), BF16), pltpu.VMEM((4, 14, 64, D), BF16), pltpu.VMEM((T, D), BF16), pltpu.VMEM((T, D), BF16),
            pltpu.VMEM((2, 448, T), BF16), pltpu.VMEM((TILES, T, WIDE), BF16), pltpu.VMEM((2, 2, ROWS, WIDE), F32), pltpu.VMEM((T, D), F32),
            pltpu.VMEM((1, 2, 8, 112, WIDE), BF16), pltpu.VMEM((4, 2, AHEAD, 64, D), BF16),
            pltpu.SemaphoreType.DMA, sems(TILES + 1), sems(2), sems(4), sems(3, BLOCKS), *GATHER_SEMS, sems(2), *[sems(7, 1)] * 2, *[sems(7, AHEAD)] * 2,
        ],
        compiler_params=pltpu.CompilerParams(collective_id=0, has_side_effects=True, vmem_limit_bytes=VMEM_LIMIT),
    )(x, w_gate, w_up, w_down)


def backward(a1, a1t, h1, dy, a0t, gu, wd0, *shards):
    pair = ((2, 2, 4, 112, WIDE), (2, 4, 64, D))
    two = ((2, 2, 2, 112, WIDE), (2, 2, 64, D))
    one = ((2, 2, 112, WIDE), (2, 64, D))
    return pl.pallas_call(
        backward_kernel,
        name="backward",
        out_shape=[shape((2, 112, FF)), shape((2, 112, FF)), shape((2, 448, D)), shape((8, 128), F32)],
        in_specs=[ANY] * 12,
        out_specs=[ANY] * 3 + [pl.BlockSpec(memory_space=pltpu.VMEM)],
        scratch_shapes=[
            pltpu.VMEM((TILES, 2, 8, 112, WIDE), BF16), pltpu.VMEM((4, 14, 64, D), BF16), pltpu.VMEM((T, D), BF16), pltpu.VMEM((2, 448, T), BF16),
            pltpu.VMEM((T, D), BF16), pltpu.VMEM((T, D), F32), *[pltpu.VMEM((T, WIDE), BF16)] * 3,
            pltpu.VMEM((SLOTS, 2, 4, 2, 112, WIDE), BF16), pltpu.VMEM((SLOTS, 4, 2, 64, D), BF16),
            *[pltpu.VMEM(dims, BF16) for dims in (*pair, *two, *one, *one, *one)],
            pltpu.VMEM((8, WIDE), F32), pltpu.VMEM((8, D), F32), pltpu.VMEM((8, 8, 128), F32),
            sems(6), sems(TILES + 1), sems(2, 2), *GATHER_SEMS,
            sems(3, 2), sems(3, 2), sems(8, 2), sems(8, 2), sems(4, 2), sems(4, 2), sems(3, 2), sems(3, 2), sems(2), sems(2), sems(2), sems(STEPS),
            sems(7), sems(7),
            *[pltpu.SemaphoreType.REGULAR] * 6,
        ],
        compiler_params=pltpu.CompilerParams(collective_id=1, has_side_effects=True, vmem_limit_bytes=VMEM_LIMIT),
    )(a1, a1t, h1, dy, a0t, gu, wd0, *shards)


def adamw(w, m, v, g):
    m = 0.9 * m + 0.1 * g
    v = 0.95 * v + 0.05 * g * g
    step = m * lax.rsqrt(v + 1e-8) + 0.1 * w
    return (w - 0.02 * step).astype(BF16), m, v


def solution(mesh):
    def step(x, dy, *arrays):
        weights, m, v = (arrays[i : i + 3] for i in (0, 3, 6))
        shards = (weights[0], weights[1], weights[2].reshape(2, 7, 64, D))
        gu, a0t, h1, a1, a1t, wd0, *ahead = forward(x[0], *shards)
        *gradients, squares = backward(a1, a1t, h1, dy[0], a0t, gu, wd0, *ahead, *shards)
        count = mesh.shape["s"] * sum(g.size for g in gradients)
        factor = jnp.minimum(1.0, 0.5 * lax.rsqrt(squares[0, 0] / count + 1e-30))
        new = [adamw(w.astype(F32), m, v, g.astype(F32) * factor) for w, m, v, g in zip(weights, m, v, gradients, strict=True)]
        return tuple(one[which] for which in range(3) for one in new)

    states, cut = P(("rep", "r", "s"), None, None), P(None, "s", None)
    return jax.shard_map(
        step,
        mesh=mesh,
        in_specs=(states, states) + (cut,) * 9,
        out_specs=(P("rep", "s", None),) * 9,
        check_vma=False,
    )
```

```python
import jax
import jax.numpy as jnp
from jax import lax
from jax.experimental import pallas as pl
from jax.experimental.pallas import tpu as pltpu
from jax.sharding import PartitionSpec as P

MESH = pl.DeviceIdType.MESH
T, D, FF = 2048, 896, 3584
TILES, WIDE, ROWS = 7, 512, 512
BLOCKS = T // ROWS
STEPS = 2 * TILES
AHEAD = 2
SLOTS = 4
OTHERS = range(1, 8)
F32, BF16 = jnp.float32, jnp.bfloat16
VMEM_LIMIT = 67_043_328
ANY = pl.BlockSpec(memory_space=pl.ANY)


def dot(a, b, contract=(1, 0)):
    return lax.dot_general(a, b, (((contract[0],), (contract[1],)), ((), ())), preferred_element_type=F32)


def loop(n, body):
    def run(i, carry):
        body(i)
        return carry

    lax.fori_loop(0, n, run, 0)


def normed(h):
    wide = h.astype(F32)
    scale = lax.rsqrt(jnp.mean(wide**2, -1, keepdims=True) + 1e-6)
    return (wide * scale).astype(BF16)


def by_owner(AT, m, a):
    turned = a.T.reshape(4, 2, 112, ROWS)
    for core in range(2):
        AT[core, :, block(m)] = turned[:, core].reshape(448, ROWS)


def block(i):
    return pl.ds(pl.multiple_of(i * ROWS, ROWS), ROWS)


def tile_of(j):
    return (j % 2) * 4 + j // 2


class Place:
    def __init__(self):
        r, s = lax.axis_index("r"), lax.axis_index("s")
        c, q = s % 2, s // 2
        y, x = q % 2, q // 2
        self.r, self.s, self.c, self.q = r, s, c, q
        dx, dy = 2 - 4 * x, 1 - 2 * y
        self.qx, self.qy, self.qd = q + dx, q + dy, q + dx + dy
        self.sx, self.sy, self.sc = s + 2 * dx, s + 2 * dy, s + 1 - 2 * c
        self.sd = s + 2 * dx + 2 * dy
        self.sa = self.sx + r * (self.sy - self.sx)
        self.sb = self.sy + r * (self.sx - self.sy)
        self.to_a, self.to_b = {"s": self.sa}, {"s": self.sb}
        self.to_x, self.to_y, self.to_c, self.to_z = {"s": self.sx}, {"s": self.sy}, {"s": self.sc}, {"r": 1 - r}

    def plane(self, n):
        return {"s": (self.s + n) % 8}


def barrier(at):
    sem = pltpu.get_barrier_semaphore()
    partners = [at.plane(n) for n in OTHERS] + [at.to_z]
    for to in partners:
        pl.semaphore_signal(sem, inc=1, device_id=to, device_id_type=MESH)
    pl.semaphore_wait(sem, len(partners))


class Gather:
    def __init__(self, at, piece, send, recv):
        self.at, self.piece, self.send, self.recv = at, piece, send, recv

    def copy(self, way, n, shard, to):
        ref = self.piece(n, shard)
        return pltpu.make_async_remote_copy(
            src_ref=ref, dst_ref=ref, send_sem=self.send.at[way, n], recv_sem=self.recv.at[way, n], device_id=to, device_id_type=MESH
        )

    def own(self, n):
        self.copy(0, n, self.at.s, self.at.to_a).start()
        self.copy(3, n, self.at.s, self.at.to_c).start()

    def first(self, n):
        at = self.at
        self.copy(0, n, at.sa, at.to_a).wait_recv()
        self.copy(1, n, at.sa, at.to_z).start()
        self.copy(2, n, at.sa, at.to_b).start()
        self.copy(4, n, at.sa, at.to_c).start()

    def second(self, n):
        at = self.at
        self.copy(1, n, at.sb, at.to_z).wait_recv()
        self.copy(5, n, at.sb, at.to_c).start()
        self.copy(2, n, at.sd, at.to_b).wait_recv()
        self.copy(6, n, at.sd, at.to_c).start()

    def whole(self, n):
        at = self.at
        across = at.sc - at.s
        for way, shard in ((3, at.s), (4, at.sa), (5, at.sb), (6, at.sd)):
            self.copy(way, n, shard + across, at.to_c).wait_recv()

    def sent(self, n):
        at = self.at
        for way, shard, to in (
            (0, at.s, at.to_a), (1, at.sa, at.to_z), (2, at.sa, at.to_b),
            (3, at.s, at.to_c), (4, at.sa, at.to_c), (5, at.sb, at.to_c), (6, at.sd, at.to_c),
        ):
            self.copy(way, n, shard, to).wait_send()


def load_tile(at, layer, j, wg_h, wu_h, into, sem):
    for which, w in enumerate((wg_h, wu_h)):
        for k in range(4):
            pltpu.make_async_copy(w.at[layer, :, pl.ds(k * 896 + tile_of(j) * 128, 128)], into.at[which, at.s, :, pl.ds(k * 128, 128)], sem).start()


def own_down(at, layer, wd_h, WD, own):
    skip = layer * AHEAD
    return pltpu.make_async_copy(wd_h.at[layer, pl.ds(skip, 7 - skip)], WD.at[at.q, pl.ds(at.c * 7 + skip, 7 - skip)], own.at[TILES])


def wait_own_tile(at, i, WGU, own):
    pltpu.make_async_copy(WGU.at[i, :, at.s], WGU.at[i, :, at.s], own.at[i]).wait()


def gathers(at, WGU, WD, sgu, rgu, sd, rd):
    gu = Gather(at, lambda n, s: WGU.at[n, :, s], sgu, rgu)
    down = Gather(at, lambda n, s: WD.at[s // 2, (s % 2) * 7 + n], sd, rd)
    return gu, down


def gate_up(WGU, i, which):
    return WGU[i, which].reshape(D, WIDE)


def down_tile(WD, j):
    return WD[:, pl.ds(2 * tile_of(j), 2)].reshape(WIDE, D)


def forward_kernel(
    x_h, wg_h, wu_h, wd_h,
    gu_o, a0t_o, h1_o, a1_o, a1t_o, wd_o, wgu1_o, wd1_o,
    WGU, WD, X, A, AT, MID, ST, ACC, WGU1, WD1,
    load, own, stage, out, done, sgu, rgu, sd, rd, own1, sgu1, rgu1, sd1, rd1,
):
    at = Place()
    for j in range(TILES):
        load_tile(at, 0, j, wg_h, wu_h, WGU.at[j], own.at[j])
    own_down(at, 0, wd_h, WD, own).start()
    load_tile(at, 1, 0, wg_h, wu_h, WGU1.at[0], own1.at[0])
    down1_in = pltpu.make_async_copy(wd_h.at[1, pl.ds(0, AHEAD)], WD1.at[at.q, at.c], own1.at[1])
    down1_in.start()
    x_in = pltpu.make_async_copy(x_h, X, load)
    x_in.start()
    barrier(at)
    gu, down = gathers(at, WGU, WD, sgu, rgu, sd, rd)
    gu1 = Gather(at, lambda n, s: WGU1.at[n, :, s], sgu1, rgu1)
    down1 = Gather(at, lambda n, s: WD1.at[s // 2, s % 2, n], sd1, rd1)

    def start_tile(n):
        wait_own_tile(at, n, WGU, own)
        gu.own(n)

    loop(TILES, start_tile)
    own_down(at, 0, wd_h, WD, own).wait()
    loop(TILES, lambda n: down.own(n))
    down1_in.wait()
    loop(AHEAD, lambda n: down1.own(n))
    wait_own_tile(at, 0, WGU1, own1)
    gu1.own(0)
    x_in.wait()

    def norm(m):
        a = normed(X[block(m), :])
        A[block(m), :] = a
        by_owner(AT, m, a)

    loop(BLOCKS, norm)
    a0t_out = pltpu.make_async_copy(AT, a0t_o, out.at[0])
    a0t_out.start()
    gu.first(0)
    gu.first(1)
    gu.second(0)

    def staged(j, m, slot):
        return pltpu.make_async_copy(ST.at[slot], gu_o.at[j, :, block(m), :], stage.at[slot])

    def tile(j):
        gu.whole(j)

        def rows(m):
            @pl.when(m == 1)
            def _():
                pl.when(j < TILES - 2)(lambda: gu.first(j + 2))
                pl.when(j >= TILES - 2)(lambda: down.first(j - TILES + 2))

            @pl.when(m == 3)
            def _():
                pl.when(j < TILES - 1)(lambda: gu.second(j + 1))
                pl.when(j == TILES - 1)(lambda: down.second(0))

            slot = m % 2
            pl.when(j * BLOCKS + m >= 2)(lambda: staged(j, m, slot).wait())
            a = A[block(m), :]
            gate = dot(a, gate_up(WGU, j, 0))
            up = dot(a, gate_up(WGU, j, 1))
            ST[slot, 0] = gate
            ST[slot, 1] = up
            staged(j, m, slot).start()
            MID[j, block(m), :] = (gate * jax.nn.sigmoid(gate) * up).astype(BF16)

        loop(BLOCKS, rows)

    loop(TILES, tile)
    down.whole(0)
    down.first(2)
    down.second(1)

    def below(j):
        down.whole(j + 1)
        pl.when(j < TILES - 3)(lambda: down.first(j + 3))

        def rows(m):
            pl.when((m == 2) & (j < TILES - 2))(lambda: down.second(j + 2))

            @pl.when((m == 2) & (j >= TILES - 3))
            def _():
                pl.when(j == TILES - 3)(lambda: down1.first(0))
                pl.when(j == TILES - 2)(lambda: down1.first(1))

            part = dot(MID[j, block(m), :], down_tile(WD, j))
            ACC[block(m), :] += part

        loop(BLOCKS, rows)

    ACC[...] = jnp.zeros_like(ACC)
    loop(TILES - 1, below)
    wd_out = pltpu.make_async_copy(WD, wd_o, out.at[1])
    wd_out.start()
    a0t_out.wait()

    gu1.first(0)
    down1.second(0)

    def finish(m):
        @pl.when(m == 2)
        def _():
            down1.second(1)
            gu1.second(0)

        total = ACC[block(m), :] + dot(MID[TILES - 1, block(m), :], down_tile(WD, TILES - 1))
        h = added(X[block(m), :], total.astype(BF16))
        X[block(m), :] = h
        a = normed(h)
        A[block(m), :] = a
        by_owner(AT, m, a)
        for one in block_out(m):
            one.start()

    def block_out(m):
        return [
            pltpu.make_async_copy(X.at[block(m), :], h1_o.at[block(m), :], done.at[0, m]),
            pltpu.make_async_copy(A.at[block(m), :], a1_o.at[block(m), :], done.at[1, m]),
            pltpu.make_async_copy(AT.at[:, :, block(m)], a1t_o.at[:, :, block(m)], done.at[2, m]),
        ]

    loop(BLOCKS, finish)
    gu1.whole(0)
    loop(AHEAD, lambda n: down1.whole(n))
    pairs = ((WGU1, wgu1_o), (WD1, wd1_o))
    outs = [pltpu.make_async_copy(v, o, out.at[2 + k]) for k, (v, o) in enumerate(pairs)]
    for o in outs:
        o.start()
    for slot in range(2):
        staged(TILES - 1, slot, slot).wait()

    def sent(n):
        gu.sent(n)
        down.sent(n)

    loop(TILES, sent)
    gu1.sent(0)
    loop(AHEAD, lambda n: down1.sent(n))
    wd_out.wait()

    def blocks_left(m):
        for one in block_out(m):
            one.wait()

    loop(BLOCKS, blocks_left)
    for o in outs:
        o.wait()


def added(a, b):
    return (a.astype(F32) + b.astype(F32)).astype(BF16)


def backward_kernel(
    a1_h, a1t_h, h1_h, dy_h, a0t_h, gu_h, wd0_h, wgu1_h, wd1_h, wg_h, wu_h, wd_h,
    gg_o, gu_o, gd_o, sq_o,
    WGU, WD, A, AT, DY, ACC, MID, DG, DU, TS, TW, TD, RW, RD, FW, FD, BW, BD, ZW, ZD, OW, OD, SQW, SQD, SQ,
    load, own, gus, sgu, rgu, sd, rd, pair_s, pair_r, first_s, first_r, second_s, second_r, z_s, z_r, ow_s, od_s, od_remote_s, od_r, sq_s, sq_r,
    pair_free, first_x, first_y, second_x, second_y, z_free,
):
    at = Place()
    c, q, qx, qy, qd = at.c, at.q, at.qx, at.qy, at.qd
    own_down(at, 1, wd_h, WD, own).start()
    for j in range(1, TILES):
        load_tile(at, 1, j, wg_h, wu_h, WGU.at[j], own.at[j])
    pairs = [(a1_h, A), (wgu1_h.at[0], WGU.at[0])]
    pairs += [(wd1_h.at[:, core], WD.at[:, pl.ds(7 * core, AHEAD)]) for core in range(2)]
    pairs += [(dy_h, DY), (a1t_h, AT)]
    loads = [pltpu.make_async_copy(h, v, load.at[k]) for k, (h, v) in enumerate(pairs)]
    for one in loads:
        one.start()
    h1_in = pltpu.make_async_copy(h1_h, A, load.at[0])
    wd0_in = pltpu.make_async_copy(wd0_h, WD, load.at[2])
    a0t_in = pltpu.make_async_copy(a0t_h, AT, load.at[3])
    barrier(at)
    gather, down = gathers(at, WGU, WD, sgu, rgu, sd, rd)
    own_down(at, 1, wd_h, WD, own).wait()

    def start_tile(j):
        down.own(j + 2)
        wait_own_tile(at, j + 1, WGU, own)
        gather.own(j + 1)

    loop(TILES - AHEAD, start_tile)
    wait_own_tile(at, TILES - 1, WGU, own)
    gather.own(TILES - 1)
    SQW[...] = jnp.zeros_like(SQW)
    SQD[...] = jnp.zeros_like(SQD)
    ACC[...] = jnp.zeros_like(ACC)
    at_in = loads.pop()
    for one in loads:
        one.wait()

    def remote(src, dst, send, recv, to):
        return pltpu.make_async_remote_copy(src_ref=src, dst_ref=dst, send_sem=send, recv_sem=recv, device_id=to, device_id_type=MESH)

    def pair_copy(t, one):
        k, j = t % SLOTS, t % 2
        src, dst = (TS.at[one], RW.at[j, one]) if one < 2 else (TD.at[k, :, 1 - c], RD.at[j])
        return remote(src, dst, pair_s.at[one, j], pair_r.at[one, j], at.to_c)

    def buffers(t, part):
        k, j = t % SLOTS, t % 2
        if part < 2:
            return (lambda p: TW.at[k, part, p]), (lambda n: FW.at[j, part, n]), BW.at[j, part]
        rows = pl.ds(32 * (part - 2), 32)
        return (lambda p: TD.at[k, p, c, rows]), (lambda n: FD.at[j, n, rows]), BD.at[j, rows]

    x, y = (at.to_x, qx), (at.to_y, qy)

    def ways(part):
        return (x, y) if part % 2 == 0 else (y, x)

    def first_copies(t, part):
        mine, into, _ = buffers(t, part)
        (to, near), _ = ways(part)
        return [remote(mine(p), into(n), first_s.at[2 * part + n, t % 2], first_r.at[2 * part + n, t % 2], to) for n, p in enumerate((near, qd))]

    def second_copy(t, part):
        mine, _, into = buffers(t, part)
        _, (to, near) = ways(part)
        return remote(mine(near), into, second_s.at[part, t % 2], second_r.at[part, t % 2], to)

    def z_copy(t, one):
        k, j = t % SLOTS, t % 2
        src, dst = (TW.at[k, one, q], ZW.at[j, one]) if one < 2 else (TD.at[k, q, c], ZD.at[j])
        return remote(src, dst, z_s.at[one, j], z_r.at[one, j], at.to_z)

    def spend(t, *sems):
        @pl.when(t >= 2)
        def _():
            for sem in sems:
                pl.semaphore_wait(sem, 1)

    def free(t, *pairs):
        @pl.when(t < STEPS - 2)
        def _():
            for sem, to in pairs:
                pl.semaphore_signal(sem, inc=1, device_id=to, device_id_type=MESH)

    PARTS = ((0,), (1,), (2, 3))

    def first_start(t, one):
        for part in PARTS[one]:
            for copy in first_copies(t, part):
                copy.start()

    def stage_one(t):
        k, j = t % SLOTS, t % 2
        pair_copy(t, 2).wait()

        def chip(p):
            TD[k, p, c] = added(TD[k, p, c], RD[j, p])

        loop(4, chip)
        first_start(t, 2)
        free(t, (pair_free, at.to_c))

    def stage_two(t):
        spend(t, second_x, second_y)
        for part in range(4):
            for copy in first_copies(t, part):
                copy.wait()
            mine, into, _ = buffers(t, part)
            _, (_, other) = ways(part)
            mine(other)[...] = added(mine(other)[...], into(1)[...])
            second_copy(t, part).start()
            mine(q)[...] = added(mine(q)[...], into(0)[...])
        free(t, (first_x, at.to_x), (first_y, at.to_y))

    def stage_three(t):
        spend(t, z_free)
        for one in range(3):
            for part in PARTS[one]:
                second_copy(t, part).wait()
                mine, _, into = buffers(t, part)
                mine(q)[...] = added(mine(q)[...], into[...])
            z_copy(t, one).start()
        free(t, (second_x, at.to_x), (second_y, at.to_y))

    def half(t, core):
        number = tile_of(t % TILES) * 2 + core
        return number // 7, pl.ds(pl.multiple_of(number % 7 * 64, 64), 64)

    def layer_of(t):
        return 1 - t // TILES

    def wide_out(t):
        j, i = t % 2, tile_of(t % TILES)
        for which, o in enumerate((gg_o, gu_o)):
            for k in range(4):
                lanes = pl.ds(pl.multiple_of(k * 896 + i * 128, 128), 128)
                yield pltpu.make_async_copy(OW.at[j, which, :, pl.ds(k * 128, 128)], o.at[layer_of(t), :, lanes], ow_s.at[j])

    def down_local(t):
        _, number = half(t, c)
        return pltpu.make_async_copy(OD.at[t % 2], gd_o.at[layer_of(t), number], od_s.at[t % 2])

    def down_remote(t, core):
        _, number = half(t, core)
        return remote(OD.at[t % 2], gd_o.at[layer_of(t), number], od_remote_s.at[t % 2], od_r.at[t], at.to_c)

    def out_start(t):
        for one in wide_out(t):
            one.start()
        owner, _ = half(t, c)
        pl.when(owner == c)(lambda: down_local(t).start())
        pl.when(owner != c)(lambda: down_remote(t, c).start())

    def out_wait(t):
        j = t % 2
        pltpu.make_async_copy(OW.at[j], OW.at[j], ow_s.at[j]).wait()
        owner, _ = half(t, c)
        pl.when(owner == c)(lambda: down_local(t).wait())
        pl.when(owner != c)(lambda: down_remote(t, c).wait_send())

    def stage_four(t):
        k, j = t % SLOTS, t % 2
        pl.when(t >= 2)(lambda: out_wait(t - 2))
        for one in range(3):
            z_copy(t, one).wait()
            g = added(TW[k, one, q], ZW[j, one]) if one < 2 else added(TD[k, q, c], ZD[j])
            wide = g.astype(F32)
            if one < 2:
                OW[j, one] = g
                SQW[...] += jnp.sum((wide * wide).reshape(14, 8, WIDE), 0)
            else:
                OD[j] = g
                SQD[...] += jnp.sum((wide * wide).reshape(8, 8, D), 0)
        free(t, (z_free, at.to_z))
        out_start(t)

    def between(gate, up, by_mid):
        sig = jax.nn.sigmoid(gate)
        silu = gate * sig
        by_gate = by_mid * up * (sig + silu * (1.0 - sig))
        return (silu * up).astype(BF16), by_gate.astype(BF16), (by_mid * silu).astype(BF16)

    def store_between(m, values):
        for ref, value in zip((MID, DG, DU), values):
            ref[block(m), :] = value

    def layer_one(i):
        pl.when((i > 0) & (i < TILES - 1))(lambda: down.whole(i + 1))
        pl.when(i > 0)(lambda: gather.whole(i))

        def rows(m):
            @pl.when((m == 2) & (i < TILES - 1))
            def _():
                pl.when(i < TILES - 2)(lambda: down.first(i + 2))
                gather.first(i + 1)

            a = A[block(m), :]
            gate = dot(a, gate_up(WGU, i, 0))
            up = dot(a, gate_up(WGU, i, 1))
            by_mid = dot(DY[block(m), :], down_tile(WD, i), (1, 1)).astype(BF16).astype(F32)
            values = between(gate, up, by_mid)
            store_between(m, values)
            ACC[block(m), :] += dot(values[1], gate_up(WGU, i, 0), (1, 1)) + dot(values[2], gate_up(WGU, i, 1), (1, 1))

        loop(BLOCKS, rows)

    def kept(n):
        i, m, slot = n // BLOCKS, n % BLOCKS, n % 2
        return [
            pltpu.make_async_copy(
                gu_h.at[i, which, block(m), :], ACC.at[pl.ds(pl.multiple_of(slot * 1024 + which * 512, 512), 512), pl.ds(0, 512)], gus.at[slot, which]
            )
            for which in range(2)
        ]

    def turn():
        a0t_in.start()
        h1_in.wait()
        wd0_in.wait()

        def rows(m):
            wide = A[block(m), :].astype(F32)
            by_a = ACC[block(m), :].astype(BF16).astype(F32)
            scale = lax.rsqrt(jnp.mean(wide**2, -1, keepdims=True) + 1e-6)
            along = jnp.mean(by_a * wide, -1, keepdims=True) * scale * scale
            by_h = (scale * (by_a - wide * along)).astype(BF16)
            DY[block(m), :] = added(DY[block(m), :], by_h)

        loop(BLOCKS, rows)
        for one in kept(0):
            one.start()

    def layer_zero(i):
        def rows(m):
            n = i * BLOCKS + m
            slot = n % 2

            @pl.when(n + 1 < TILES * BLOCKS)
            def _():
                for one in kept(n + 1):
                    one.start()

            for one in kept(n):
                one.wait()
            gate, up = (ACC[pl.ds(pl.multiple_of(slot * 1024 + which * 512, 512), 512), pl.ds(0, 512)] for which in range(2))
            by_mid = dot(DY[block(m), :], down_tile(WD, i), (1, 1)).astype(BF16).astype(F32)
            store_between(m, between(gate, up, by_mid))

        loop(BLOCKS, rows)

    def gradients(t):
        k, j = t % SLOTS, t % 2
        spend(t, pair_free)
        for which, by in enumerate((DG, DU)):
            TS[which] = dot(AT[1 - c], by[...]).astype(BF16).reshape(4, 112, WIDE)
            pair_copy(t, which).start()
        TD[k] = dot(MID[...], DY[...], (0, 0)).astype(BF16).reshape(4, 2, 64, D)
        pair_copy(t, 2).start()
        spend(t, first_x, first_y)
        for which, by in enumerate((DG, DU)):
            pair_copy(t, which).wait()
            TW[k, which] = (dot(AT[c], by[...]).reshape(4, 112, WIDE) + RW[j, which].astype(F32)).astype(BF16)
            first_start(t, which)

    def step(t):
        pl.when(t < TILES)(lambda: layer_one(t))
        pl.when(t == TILES)(turn)
        pl.when((t >= TILES) & (t < STEPS))(lambda: layer_zero(t - TILES))

        pl.when((t >= 1) & (t <= STEPS))(lambda: stage_one(t - 1))
        pl.when((t >= 3) & (t <= STEPS + 2))(lambda: stage_three(t - 3))
        pl.when((t >= 2) & (t <= STEPS + 1))(lambda: stage_two(t - 2))
        pl.when(t >= 4)(lambda: stage_four(t - 4))

        @pl.when(t < TILES - 1)
        def _():
            pl.when(t < TILES - 2)(lambda: down.second(t + 2))
            gather.second(t + 1)

        @pl.when(t == TILES - 1)
        def _():
            h1_in.start()
            loop(TILES - AHEAD, lambda n: down.sent(n + AHEAD))
            wd0_in.start()

        pl.when(t == 0)(at_in.wait)
        pl.when(t == TILES)(a0t_in.wait)
        pl.when(t < STEPS)(lambda: gradients(t))

    loop(STEPS + 4, step)

    mine = jnp.sum(SQW[...], keepdims=True) + jnp.sum(SQD[...], keepdims=True)
    SQ[at.s] = jnp.broadcast_to(mine, (8, 128))

    def square(n, from_):
        return remote(SQ.at[from_], SQ.at[from_], sq_s.at[n - 1], sq_r.at[n - 1], at.plane(n))

    for n in OTHERS:
        square(n, at.s).start()
    out_wait(STEPS - 2)
    out_wait(STEPS - 1)

    loop(TILES - 1, lambda n: gather.sent(n + 1))

    def arrived(t):
        owner, _ = half(t, 1 - c)
        pl.when(owner == c)(lambda: down_remote(t, 1 - c).wait_recv())

    loop(STEPS, arrived)
    for n in OTHERS:
        square(n, (at.s + 8 - n) % 8).wait_recv()
        square(n, at.s).wait_send()
    total = SQ[0]
    for n in OTHERS:
        total += SQ[n]
    sq_o[...] = total


def shape(dims, dtype=BF16):
    return jax.ShapeDtypeStruct(dims, dtype)


def sems(*dims):
    return pltpu.SemaphoreType.DMA(dims)


GATHER_SEMS = [sems(7, TILES)] * 4


def forward(x, w_gate, w_up, w_down):
    return pl.pallas_call(
        forward_kernel,
        name="forward",
        out_shape=[
            shape((TILES, 2, T, WIDE), F32), shape((2, 448, T)), shape((T, D)), shape((T, D)), shape((2, 448, T)), shape((4, 14, 64, D)),
            shape((1, 2, 8, 112, WIDE)), shape((4, 2, AHEAD, 64, D)),
        ],
        in_specs=[ANY] * 4,
        out_specs=[ANY] * 8,
        scratch_shapes=[
            pltpu.VMEM((TILES, 2, 8, 112, WIDE), BF16), pltpu.VMEM((4, 14, 64, D), BF16), pltpu.VMEM((T, D), BF16), pltpu.VMEM((T, D), BF16),
            pltpu.VMEM((2, 448, T), BF16), pltpu.VMEM((TILES, T, WIDE), BF16), pltpu.VMEM((2, 2, ROWS, WIDE), F32), pltpu.VMEM((T, D), F32),
            pltpu.VMEM((1, 2, 8, 112, WIDE), BF16), pltpu.VMEM((4, 2, AHEAD, 64, D), BF16),
            pltpu.SemaphoreType.DMA, sems(TILES + 1), sems(2), sems(4), sems(3, BLOCKS), *GATHER_SEMS, sems(2), *[sems(7, 1)] * 2, *[sems(7, AHEAD)] * 2,
        ],
        compiler_params=pltpu.CompilerParams(collective_id=0, has_side_effects=True, vmem_limit_bytes=VMEM_LIMIT),
    )(x, w_gate, w_up, w_down)


def backward(a1, a1t, h1, dy, a0t, gu, wd0, *shards):
    pair = ((2, 2, 4, 112, WIDE), (2, 4, 64, D))
    two = ((2, 2, 2, 112, WIDE), (2, 2, 64, D))
    one = ((2, 2, 112, WIDE), (2, 64, D))
    return pl.pallas_call(
        backward_kernel,
        name="backward",
        out_shape=[shape((2, 112, FF)), shape((2, 112, FF)), shape((2, 448, D)), shape((8, 128), F32)],
        in_specs=[ANY] * 12,
        out_specs=[ANY] * 3 + [pl.BlockSpec(memory_space=pltpu.VMEM)],
        scratch_shapes=[
            pltpu.VMEM((TILES, 2, 8, 112, WIDE), BF16), pltpu.VMEM((4, 14, 64, D), BF16), pltpu.VMEM((T, D), BF16), pltpu.VMEM((2, 448, T), BF16),
            pltpu.VMEM((T, D), BF16), pltpu.VMEM((T, D), F32), *[pltpu.VMEM((T, WIDE), BF16)] * 3,
            pltpu.VMEM((2, 4, 112, WIDE), BF16), pltpu.VMEM((SLOTS, 2, 4, 112, WIDE), BF16), pltpu.VMEM((SLOTS, 4, 2, 64, D), BF16),
            *[pltpu.VMEM(dims, BF16) for dims in (*pair, *two, *one, *one, *one)],
            pltpu.VMEM((8, WIDE), F32), pltpu.VMEM((8, D), F32), pltpu.VMEM((8, 8, 128), F32),
            sems(6), sems(TILES + 1), sems(2, 2), *GATHER_SEMS,
            sems(3, 2), sems(3, 2), sems(8, 2), sems(8, 2), sems(4, 2), sems(4, 2), sems(3, 2), sems(3, 2), sems(2), sems(2), sems(2), sems(STEPS),
            sems(7), sems(7),
            *[pltpu.SemaphoreType.REGULAR] * 6,
        ],
        compiler_params=pltpu.CompilerParams(collective_id=1, has_side_effects=True, vmem_limit_bytes=VMEM_LIMIT),
    )(a1, a1t, h1, dy, a0t, gu, wd0, *shards)


def adamw(w, m, v, g):
    m = 0.9 * m + 0.1 * g
    v = 0.95 * v + 0.05 * g * g
    step = m * lax.rsqrt(v + 1e-8) + 0.1 * w
    return (w - 0.02 * step).astype(BF16), m, v


def solution(mesh):
    def step(x, dy, *arrays):
        weights, m, v = (arrays[i : i + 3] for i in (0, 3, 6))
        shards = (weights[0], weights[1], weights[2].reshape(2, 7, 64, D))
        gu, a0t, h1, a1, a1t, wd0, *ahead = forward(x[0], *shards)
        *gradients, squares = backward(a1, a1t, h1, dy[0], a0t, gu, wd0, *ahead, *shards)
        count = mesh.shape["s"] * sum(g.size for g in gradients)
        factor = jnp.minimum(1.0, 0.5 * lax.rsqrt(squares[0, 0] / count + 1e-30))
        new = [adamw(w.astype(F32), m, v, g.astype(F32) * factor) for w, m, v, g in zip(weights, m, v, gradients, strict=True)]
        return tuple(one[which] for which in range(3) for one in new)

    states, cut = P(("rep", "r", "s"), None, None), P(None, "s", None)
    return jax.shard_map(
        step,
        mesh=mesh,
        in_specs=(states, states) + (cut,) * 9,
        out_specs=(P("rep", "s", None),) * 9,
        check_vma=False,
    )
```

```python
import jax
import jax.numpy as jnp
from jax import lax
from jax.experimental import pallas as pl
from jax.experimental.pallas import tpu as pltpu
from jax.sharding import PartitionSpec as P

MESH = pl.DeviceIdType.MESH
T, D, FF = 2048, 896, 3584
TILES, WIDE, ROWS = 7, 512, 512
BLOCKS = T // ROWS
STEPS = 2 * TILES
AHEAD = 2
SLOTS = 4
OTHERS = range(1, 8)
F32, BF16 = jnp.float32, jnp.bfloat16
VMEM_LIMIT = 67_043_328
ANY = pl.BlockSpec(memory_space=pl.ANY)


def dot(a, b, contract=(1, 0)):
    return lax.dot_general(a, b, (((contract[0],), (contract[1],)), ((), ())), preferred_element_type=F32)


def loop(n, body):
    def run(i, carry):
        body(i)
        return carry

    lax.fori_loop(0, n, run, 0)


def normed(h):
    wide = h.astype(F32)
    scale = lax.rsqrt(jnp.mean(wide**2, -1, keepdims=True) + 1e-6)
    return (wide * scale).astype(BF16)


def by_owner(AT, m, a):
    turned = a.T.reshape(4, 2, 112, ROWS)
    for core in range(2):
        AT[core, :, block(m)] = turned[:, core].reshape(448, ROWS)


def block(i):
    return pl.ds(pl.multiple_of(i * ROWS, ROWS), ROWS)


def tile_of(j):
    return (j % 2) * 4 + j // 2


class Place:
    def __init__(self):
        r, s = lax.axis_index("r"), lax.axis_index("s")
        c, q = s % 2, s // 2
        y, x = q % 2, q // 2
        self.r, self.s, self.c, self.q = r, s, c, q
        dx, dy = 2 - 4 * x, 1 - 2 * y
        self.qx, self.qy, self.qd = q + dx, q + dy, q + dx + dy
        self.sx, self.sy, self.sc = s + 2 * dx, s + 2 * dy, s + 1 - 2 * c
        self.sd = s + 2 * dx + 2 * dy
        self.sa = self.sx + r * (self.sy - self.sx)
        self.sb = self.sy + r * (self.sx - self.sy)
        self.to_a, self.to_b = {"s": self.sa}, {"s": self.sb}
        self.to_x, self.to_y, self.to_c, self.to_z = {"s": self.sx}, {"s": self.sy}, {"s": self.sc}, {"r": 1 - r}

    def plane(self, n):
        return {"s": (self.s + n) % 8}


def barrier(at):
    sem = pltpu.get_barrier_semaphore()
    partners = [at.plane(n) for n in OTHERS] + [at.to_z]
    for to in partners:
        pl.semaphore_signal(sem, inc=1, device_id=to, device_id_type=MESH)
    pl.semaphore_wait(sem, len(partners))


class Gather:
    def __init__(self, at, piece, send, recv):
        self.at, self.piece, self.send, self.recv = at, piece, send, recv

    def copy(self, way, n, shard, to):
        ref = self.piece(n, shard)
        return pltpu.make_async_remote_copy(
            src_ref=ref, dst_ref=ref, send_sem=self.send.at[way, n], recv_sem=self.recv.at[way, n], device_id=to, device_id_type=MESH
        )

    def own(self, n):
        self.copy(0, n, self.at.s, self.at.to_a).start()
        self.copy(3, n, self.at.s, self.at.to_c).start()

    def first(self, n):
        at = self.at
        self.copy(0, n, at.sa, at.to_a).wait_recv()
        self.copy(1, n, at.sa, at.to_z).start()
        self.copy(2, n, at.sa, at.to_b).start()
        self.copy(4, n, at.sa, at.to_c).start()

    def second(self, n):
        at = self.at
        self.copy(1, n, at.sb, at.to_z).wait_recv()
        self.copy(5, n, at.sb, at.to_c).start()
        self.copy(2, n, at.sd, at.to_b).wait_recv()
        self.copy(6, n, at.sd, at.to_c).start()

    def whole(self, n):
        at = self.at
        across = at.sc - at.s
        for way, shard in ((3, at.s), (4, at.sa), (5, at.sb), (6, at.sd)):
            self.copy(way, n, shard + across, at.to_c).wait_recv()

    def sent(self, n):
        at = self.at
        for way, shard, to in (
            (0, at.s, at.to_a), (1, at.sa, at.to_z), (2, at.sa, at.to_b),
            (3, at.s, at.to_c), (4, at.sa, at.to_c), (5, at.sb, at.to_c), (6, at.sd, at.to_c),
        ):
            self.copy(way, n, shard, to).wait_send()


def load_tile(at, layer, j, wg_h, wu_h, into, sem):
    for which, w in enumerate((wg_h, wu_h)):
        for k in range(4):
            pltpu.make_async_copy(w.at[layer, :, pl.ds(k * 896 + tile_of(j) * 128, 128)], into.at[which, at.s, :, pl.ds(k * 128, 128)], sem).start()


def own_down(at, layer, wd_h, WD, own):
    skip = layer * AHEAD
    return pltpu.make_async_copy(wd_h.at[layer, pl.ds(skip, 7 - skip)], WD.at[at.q, pl.ds(at.c * 7 + skip, 7 - skip)], own.at[TILES])


def wait_own_tile(at, i, WGU, own):
    pltpu.make_async_copy(WGU.at[i, :, at.s], WGU.at[i, :, at.s], own.at[i]).wait()


def gathers(at, WGU, WD, sgu, rgu, sd, rd):
    gu = Gather(at, lambda n, s: WGU.at[n, :, s], sgu, rgu)
    down = Gather(at, lambda n, s: WD.at[s // 2, (s % 2) * 7 + n], sd, rd)
    return gu, down


def gate_up(WGU, i, which):
    return WGU[i, which].reshape(D, WIDE)


def down_tile(WD, j):
    return WD[:, pl.ds(2 * tile_of(j), 2)].reshape(WIDE, D)


def forward_kernel(
    x_h, wg_h, wu_h, wd_h,
    gu_o, a0t_o, h1_o, a1_o, a1t_o, wd_o, wgu1_o, wd1_o,
    WGU, WD, X, A, AT, MID, ST, ACC, WGU1, WD1,
    load, own, stage, out, done, sgu, rgu, sd, rd, own1, sgu1, rgu1, sd1, rd1,
):
    at = Place()
    for j in range(TILES):
        load_tile(at, 0, j, wg_h, wu_h, WGU.at[j], own.at[j])
    own_down(at, 0, wd_h, WD, own).start()
    load_tile(at, 1, 0, wg_h, wu_h, WGU1.at[0], own1.at[0])
    down1_in = pltpu.make_async_copy(wd_h.at[1, pl.ds(0, AHEAD)], WD1.at[at.q, at.c], own1.at[1])
    down1_in.start()
    x_in = pltpu.make_async_copy(x_h, X, load)
    x_in.start()
    barrier(at)
    gu, down = gathers(at, WGU, WD, sgu, rgu, sd, rd)
    gu1 = Gather(at, lambda n, s: WGU1.at[n, :, s], sgu1, rgu1)
    down1 = Gather(at, lambda n, s: WD1.at[s // 2, s % 2, n], sd1, rd1)

    def start_tile(n):
        wait_own_tile(at, n, WGU, own)
        gu.own(n)

    loop(TILES, start_tile)
    own_down(at, 0, wd_h, WD, own).wait()
    loop(TILES, lambda n: down.own(n))
    down1_in.wait()
    loop(AHEAD, lambda n: down1.own(n))
    wait_own_tile(at, 0, WGU1, own1)
    gu1.own(0)
    x_in.wait()

    def norm(m):
        a = normed(X[block(m), :])
        A[block(m), :] = a
        by_owner(AT, m, a)

    loop(BLOCKS, norm)
    a0t_out = pltpu.make_async_copy(AT, a0t_o, out.at[0])
    a0t_out.start()
    gu.first(0)
    gu.first(1)
    gu.second(0)

    def staged(j, m, slot):
        return pltpu.make_async_copy(ST.at[slot], gu_o.at[j, :, block(m), :], stage.at[slot])

    def tile(j):
        gu.whole(j)

        def rows(m):
            @pl.when(m == 1)
            def _():
                pl.when(j < TILES - 2)(lambda: gu.first(j + 2))
                pl.when(j >= TILES - 2)(lambda: down.first(j - TILES + 2))

            @pl.when(m == 3)
            def _():
                pl.when(j < TILES - 1)(lambda: gu.second(j + 1))
                pl.when(j == TILES - 1)(lambda: down.second(0))

            slot = m % 2
            pl.when(j * BLOCKS + m >= 2)(lambda: staged(j, m, slot).wait())
            a = A[block(m), :]
            gate = dot(a, gate_up(WGU, j, 0))
            up = dot(a, gate_up(WGU, j, 1))
            ST[slot, 0] = gate
            ST[slot, 1] = up
            staged(j, m, slot).start()
            MID[j, block(m), :] = (gate * jax.nn.sigmoid(gate) * up).astype(BF16)

        loop(BLOCKS, rows)

    loop(TILES, tile)
    down.whole(0)
    down.first(2)
    down.second(1)

    def below(j):
        down.whole(j + 1)
        pl.when(j < TILES - 3)(lambda: down.first(j + 3))

        def rows(m):
            pl.when((m == 2) & (j < TILES - 2))(lambda: down.second(j + 2))

            @pl.when((m == 2) & (j >= TILES - 3))
            def _():
                pl.when(j == TILES - 3)(lambda: down1.first(0))
                pl.when(j == TILES - 2)(lambda: down1.first(1))

            part = dot(MID[j, block(m), :], down_tile(WD, j))
            ACC[block(m), :] += part

        loop(BLOCKS, rows)

    ACC[...] = jnp.zeros_like(ACC)
    loop(TILES - 1, below)
    wd_out = pltpu.make_async_copy(WD, wd_o, out.at[1])
    wd_out.start()
    a0t_out.wait()

    gu1.first(0)
    down1.second(0)

    def finish(m):
        @pl.when(m == 2)
        def _():
            down1.second(1)
            gu1.second(0)

        total = ACC[block(m), :] + dot(MID[TILES - 1, block(m), :], down_tile(WD, TILES - 1))
        h = added(X[block(m), :], total.astype(BF16))
        X[block(m), :] = h
        a = normed(h)
        A[block(m), :] = a
        by_owner(AT, m, a)
        for one in block_out(m):
            one.start()

    def block_out(m):
        return [
            pltpu.make_async_copy(X.at[block(m), :], h1_o.at[block(m), :], done.at[0, m]),
            pltpu.make_async_copy(A.at[block(m), :], a1_o.at[block(m), :], done.at[1, m]),
            pltpu.make_async_copy(AT.at[:, :, block(m)], a1t_o.at[:, :, block(m)], done.at[2, m]),
        ]

    loop(BLOCKS, finish)
    gu1.whole(0)
    loop(AHEAD, lambda n: down1.whole(n))
    pairs = ((WGU1, wgu1_o), (WD1, wd1_o))
    outs = [pltpu.make_async_copy(v, o, out.at[2 + k]) for k, (v, o) in enumerate(pairs)]
    for o in outs:
        o.start()
    for slot in range(2):
        staged(TILES - 1, slot, slot).wait()

    def sent(n):
        gu.sent(n)
        down.sent(n)

    loop(TILES, sent)
    gu1.sent(0)
    loop(AHEAD, lambda n: down1.sent(n))
    wd_out.wait()

    def blocks_left(m):
        for one in block_out(m):
            one.wait()

    loop(BLOCKS, blocks_left)
    for o in outs:
        o.wait()


def added(a, b):
    return (a.astype(F32) + b.astype(F32)).astype(BF16)


def backward_kernel(
    a1_h, a1t_h, h1_h, dy_h, a0t_h, gu_h, wd0_h, wgu1_h, wd1_h, wg_h, wu_h, wd_h,
    gg_o, gu_o, gd_o, sq_o,
    WGU, WD, A, AT, DY, ACC, MID, DG, DU, TS, TW, TD, RW, RD, FW, FD, BW, BD, ZW, ZD, OW, OD, SQW, SQD, SQ,
    load, own, gus, sgu, rgu, sd, rd, pair_s, pair_r, first_s, first_r, second_s, second_r, z_s, z_r, ow_s, od_s, od_remote_s, od_r, sq_s, sq_r,
    pair_free, first_x, first_y, second_x, second_y, z_free,
):
    at = Place()
    c, q, qx, qy, qd = at.c, at.q, at.qx, at.qy, at.qd
    own_down(at, 1, wd_h, WD, own).start()
    for j in range(1, TILES):
        load_tile(at, 1, j, wg_h, wu_h, WGU.at[j], own.at[j])
    pairs = [(a1_h, A), (wgu1_h.at[0], WGU.at[0])]
    pairs += [(wd1_h.at[:, core], WD.at[:, pl.ds(7 * core, AHEAD)]) for core in range(2)]
    pairs += [(dy_h, DY), (a1t_h, AT)]
    loads = [pltpu.make_async_copy(h, v, load.at[k]) for k, (h, v) in enumerate(pairs)]
    for one in loads:
        one.start()
    h1_in = pltpu.make_async_copy(h1_h, A, load.at[0])
    wd0_in = pltpu.make_async_copy(wd0_h, WD, load.at[2])
    a0t_in = pltpu.make_async_copy(a0t_h, AT, load.at[3])
    barrier(at)
    gather, down = gathers(at, WGU, WD, sgu, rgu, sd, rd)
    own_down(at, 1, wd_h, WD, own).wait()

    def start_tile(j):
        down.own(j + 2)
        wait_own_tile(at, j + 1, WGU, own)
        gather.own(j + 1)

    loop(TILES - AHEAD, start_tile)
    wait_own_tile(at, TILES - 1, WGU, own)
    gather.own(TILES - 1)
    SQW[...] = jnp.zeros_like(SQW)
    SQD[...] = jnp.zeros_like(SQD)
    ACC[...] = jnp.zeros_like(ACC)
    at_in = loads.pop()
    for one in loads:
        one.wait()

    def remote(src, dst, send, recv, to):
        return pltpu.make_async_remote_copy(src_ref=src, dst_ref=dst, send_sem=send, recv_sem=recv, device_id=to, device_id_type=MESH)

    def pair_copy(t, one):
        k, j = t % SLOTS, t % 2
        src, dst = (TS.at[one], RW.at[j, one]) if one < 2 else (TD.at[k, :, 1 - c], RD.at[j])
        return remote(src, dst, pair_s.at[one, j], pair_r.at[one, j], at.to_c)

    def buffers(t, part):
        k, j = t % SLOTS, t % 2
        if part < 2:
            return (lambda p: TW.at[k, part, p]), (lambda n: FW.at[j, part, n]), BW.at[j, part]
        rows = pl.ds(32 * (part - 2), 32)
        return (lambda p: TD.at[k, p, c, rows]), (lambda n: FD.at[j, n, rows]), BD.at[j, rows]

    x, y = (at.to_x, qx), (at.to_y, qy)

    def ways(part):
        return (x, y) if part % 2 == 0 else (y, x)

    def first_copies(t, part):
        mine, into, _ = buffers(t, part)
        (to, near), _ = ways(part)
        return [remote(mine(p), into(n), first_s.at[2 * part + n, t % 2], first_r.at[2 * part + n, t % 2], to) for n, p in enumerate((near, qd))]

    def second_copy(t, part):
        mine, _, into = buffers(t, part)
        _, (to, near) = ways(part)
        return remote(mine(near), into, second_s.at[part, t % 2], second_r.at[part, t % 2], to)

    def z_copy(t, one):
        k, j = t % SLOTS, t % 2
        src, dst = (TW.at[k, one, q], ZW.at[j, one]) if one < 2 else (TD.at[k, q, c], ZD.at[j])
        return remote(src, dst, z_s.at[one, j], z_r.at[one, j], at.to_z)

    def spend(t, *sems):
        @pl.when(t >= 2)
        def _():
            for sem in sems:
                pl.semaphore_wait(sem, 1)

    def free(t, *pairs):
        @pl.when(t < STEPS - 2)
        def _():
            for sem, to in pairs:
                pl.semaphore_signal(sem, inc=1, device_id=to, device_id_type=MESH)

    PARTS = ((0,), (1,), (2, 3))

    def first_start(t, one):
        for part in PARTS[one]:
            for copy in first_copies(t, part):
                copy.start()

    def stage_one(t):
        k, j = t % SLOTS, t % 2
        pair_copy(t, 2).wait()

        def chip(p):
            TD[k, p, c] = added(TD[k, p, c], RD[j, p])

        loop(4, chip)
        first_start(t, 2)
        free(t, (pair_free, at.to_c))

    def stage_two(t):
        spend(t, second_x, second_y)
        for part in range(4):
            for copy in first_copies(t, part):
                copy.wait()
            mine, into, _ = buffers(t, part)
            _, (_, other) = ways(part)
            mine(other)[...] = added(mine(other)[...], into(1)[...])
            second_copy(t, part).start()
            mine(q)[...] = added(mine(q)[...], into(0)[...])
        free(t, (first_x, at.to_x), (first_y, at.to_y))

    def stage_three(t):
        spend(t, z_free)
        for one in range(3):
            for part in PARTS[one]:
                second_copy(t, part).wait()
                mine, _, into = buffers(t, part)
                mine(q)[...] = added(mine(q)[...], into[...])
            z_copy(t, one).start()
        free(t, (second_x, at.to_x), (second_y, at.to_y))

    def half(t, core):
        number = tile_of(t % TILES) * 2 + core
        return number // 7, pl.ds(pl.multiple_of(number % 7 * 64, 64), 64)

    def layer_of(t):
        return 1 - t // TILES

    def wide_out(t):
        j, i = t % 2, tile_of(t % TILES)
        for which, o in enumerate((gg_o, gu_o)):
            for k in range(4):
                lanes = pl.ds(pl.multiple_of(k * 896 + i * 128, 128), 128)
                yield pltpu.make_async_copy(OW.at[j, which, :, pl.ds(k * 128, 128)], o.at[layer_of(t), :, lanes], ow_s.at[j])

    def down_local(t):
        _, number = half(t, c)
        return pltpu.make_async_copy(OD.at[t % 2], gd_o.at[layer_of(t), number], od_s.at[t % 2])

    def down_remote(t, core):
        _, number = half(t, core)
        return remote(OD.at[t % 2], gd_o.at[layer_of(t), number], od_remote_s.at[t % 2], od_r.at[t], at.to_c)

    def out_start(t):
        for one in wide_out(t):
            one.start()
        owner, _ = half(t, c)
        pl.when(owner == c)(lambda: down_local(t).start())
        pl.when(owner != c)(lambda: down_remote(t, c).start())

    def out_wait(t):
        j = t % 2
        pltpu.make_async_copy(OW.at[j], OW.at[j], ow_s.at[j]).wait()
        owner, _ = half(t, c)
        pl.when(owner == c)(lambda: down_local(t).wait())
        pl.when(owner != c)(lambda: down_remote(t, c).wait_send())

    def stage_four(t):
        k, j = t % SLOTS, t % 2
        pl.when(t >= 2)(lambda: out_wait(t - 2))
        for one in range(3):
            z_copy(t, one).wait()
            g = added(TW[k, one, q], ZW[j, one]) if one < 2 else added(TD[k, q, c], ZD[j])
            wide = g.astype(F32)
            if one < 2:
                OW[j, one] = g
                SQW[...] += jnp.sum((wide * wide).reshape(14, 8, WIDE), 0)
            else:
                OD[j] = g
                SQD[...] += jnp.sum((wide * wide).reshape(8, 8, D), 0)
        free(t, (z_free, at.to_z))
        out_start(t)

    def between(gate, up, by_mid):
        sig = jax.nn.sigmoid(gate)
        silu = gate * sig
        by_gate = by_mid * up * (sig + silu * (1.0 - sig))
        return (silu * up).astype(BF16), by_gate.astype(BF16), (by_mid * silu).astype(BF16)

    def store_between(m, values):
        for ref, value in zip((MID, DG, DU), values):
            ref[block(m), :] = value

    def layer_one(i):
        pl.when((i > 0) & (i < TILES - 1))(lambda: down.whole(i + 1))
        pl.when(i > 0)(lambda: gather.whole(i))

        def rows(m):
            @pl.when((m == 2) & (i < TILES - 1))
            def _():
                pl.when(i < TILES - 2)(lambda: down.first(i + 2))
                gather.first(i + 1)

            a = A[block(m), :]
            gate = dot(a, gate_up(WGU, i, 0))
            up = dot(a, gate_up(WGU, i, 1))
            by_mid = dot(DY[block(m), :], down_tile(WD, i), (1, 1)).astype(BF16).astype(F32)
            values = between(gate, up, by_mid)
            store_between(m, values)
            ACC[block(m), :] += dot(values[1], gate_up(WGU, i, 0), (1, 1)) + dot(values[2], gate_up(WGU, i, 1), (1, 1))

        loop(BLOCKS, rows)

    def kept(n):
        i, m, slot = n // BLOCKS, n % BLOCKS, n % 2
        return [
            pltpu.make_async_copy(
                gu_h.at[i, which, block(m), :], ACC.at[pl.ds(pl.multiple_of(slot * 1024 + which * 512, 512), 512), pl.ds(0, 512)], gus.at[slot, which]
            )
            for which in range(2)
        ]

    def turn():
        a0t_in.start()
        h1_in.wait()
        wd0_in.wait()

        def rows(m):
            wide = A[block(m), :].astype(F32)
            by_a = ACC[block(m), :].astype(BF16).astype(F32)
            scale = lax.rsqrt(jnp.mean(wide**2, -1, keepdims=True) + 1e-6)
            along = jnp.mean(by_a * wide, -1, keepdims=True) * scale * scale
            by_h = (scale * (by_a - wide * along)).astype(BF16)
            DY[block(m), :] = added(DY[block(m), :], by_h)

        loop(BLOCKS, rows)
        for one in kept(0):
            one.start()

    def layer_zero(i):
        def rows(m):
            n = i * BLOCKS + m
            slot = n % 2

            @pl.when(n + 1 < TILES * BLOCKS)
            def _():
                for one in kept(n + 1):
                    one.start()

            for one in kept(n):
                one.wait()
            gate, up = (ACC[pl.ds(pl.multiple_of(slot * 1024 + which * 512, 512), 512), pl.ds(0, 512)] for which in range(2))
            by_mid = dot(DY[block(m), :], down_tile(WD, i), (1, 1)).astype(BF16).astype(F32)
            store_between(m, between(gate, up, by_mid))

        loop(BLOCKS, rows)

    def gradients(t):
        k, j = t % SLOTS, t % 2
        spend(t, pair_free)
        for which, by in enumerate((DG, DU)):
            TS[which] = dot(AT[1 - c], by[...]).astype(BF16).reshape(4, 112, WIDE)
            pair_copy(t, which).start()
        TD[k] = dot(MID[...], DY[...], (0, 0)).astype(BF16).reshape(4, 2, 64, D)
        pair_copy(t, 2).start()
        spend(t, first_x, first_y)
        for which, by in enumerate((DG, DU)):
            pair_copy(t, which).wait()
            TW[k, which] = (dot(AT[c], by[...]).reshape(4, 112, WIDE) + RW[j, which].astype(F32)).astype(BF16)
            first_start(t, which)

    def step(t):
        pl.when(t < TILES)(lambda: layer_one(t))
        pl.when(t == TILES)(turn)
        pl.when((t >= TILES) & (t < STEPS))(lambda: layer_zero(t - TILES))

        pl.when((t >= 1) & (t <= STEPS))(lambda: stage_one(t - 1))
        pl.when((t >= 3) & (t <= STEPS + 2))(lambda: stage_three(t - 3))
        pl.when((t >= 2) & (t <= STEPS + 1))(lambda: stage_two(t - 2))
        pl.when(t >= 4)(lambda: stage_four(t - 4))

        @pl.when(t < TILES - 1)
        def _():
            pl.when(t < TILES - 2)(lambda: down.second(t + 2))
            gather.second(t + 1)

        @pl.when(t == TILES - 1)
        def _():
            h1_in.start()
            loop(TILES - AHEAD, lambda n: down.sent(n + AHEAD))
            wd0_in.start()

        pl.when(t == 0)(at_in.wait)
        pl.when(t == TILES)(a0t_in.wait)
        pl.when(t < STEPS)(lambda: gradients(t))

    loop(STEPS + 4, step)

    mine = jnp.sum(SQW[...], keepdims=True) + jnp.sum(SQD[...], keepdims=True)
    SQ[at.s] = jnp.broadcast_to(mine, (8, 128))

    def square(n, from_):
        return remote(SQ.at[from_], SQ.at[from_], sq_s.at[n - 1], sq_r.at[n - 1], at.plane(n))

    for n in OTHERS:
        square(n, at.s).start()
    out_wait(STEPS - 2)
    out_wait(STEPS - 1)

    loop(TILES - 1, lambda n: gather.sent(n + 1))

    def arrived(t):
        owner, _ = half(t, 1 - c)
        pl.when(owner == c)(lambda: down_remote(t, 1 - c).wait_recv())

    loop(STEPS, arrived)
    for n in OTHERS:
        square(n, (at.s + 8 - n) % 8).wait_recv()
        square(n, at.s).wait_send()
    total = SQ[0]
    for n in OTHERS:
        total += SQ[n]
    sq_o[0, 0] = jnp.sum(total[:1, :1])


def shape(dims, dtype=BF16):
    return jax.ShapeDtypeStruct(dims, dtype)


def sems(*dims):
    return pltpu.SemaphoreType.DMA(dims)


GATHER_SEMS = [sems(7, TILES)] * 4


def forward(x, w_gate, w_up, w_down):
    return pl.pallas_call(
        forward_kernel,
        name="forward",
        out_shape=[
            shape((TILES, 2, T, WIDE), F32), shape((2, 448, T)), shape((T, D)), shape((T, D)), shape((2, 448, T)), shape((4, 14, 64, D)),
            shape((1, 2, 8, 112, WIDE)), shape((4, 2, AHEAD, 64, D)),
        ],
        in_specs=[ANY] * 4,
        out_specs=[ANY] * 8,
        scratch_shapes=[
            pltpu.VMEM((TILES, 2, 8, 112, WIDE), BF16), pltpu.VMEM((4, 14, 64, D), BF16), pltpu.VMEM((T, D), BF16), pltpu.VMEM((T, D), BF16),
            pltpu.VMEM((2, 448, T), BF16), pltpu.VMEM((TILES, T, WIDE), BF16), pltpu.VMEM((2, 2, ROWS, WIDE), F32), pltpu.VMEM((T, D), F32),
            pltpu.VMEM((1, 2, 8, 112, WIDE), BF16), pltpu.VMEM((4, 2, AHEAD, 64, D), BF16),
            pltpu.SemaphoreType.DMA, sems(TILES + 1), sems(2), sems(4), sems(3, BLOCKS), *GATHER_SEMS, sems(2), *[sems(7, 1)] * 2, *[sems(7, AHEAD)] * 2,
        ],
        compiler_params=pltpu.CompilerParams(collective_id=0, has_side_effects=True, vmem_limit_bytes=VMEM_LIMIT),
    )(x, w_gate, w_up, w_down)


def backward(a1, a1t, h1, dy, a0t, gu, wd0, *shards):
    pair = ((2, 2, 4, 112, WIDE), (2, 4, 64, D))
    two = ((2, 2, 2, 112, WIDE), (2, 2, 64, D))
    one = ((2, 2, 112, WIDE), (2, 64, D))
    return pl.pallas_call(
        backward_kernel,
        name="backward",
        out_shape=[shape((2, 112, FF)), shape((2, 112, FF)), shape((2, 448, D)), shape((1, 1), F32)],
        in_specs=[ANY] * 12,
        out_specs=[ANY] * 3 + [pl.BlockSpec(memory_space=pltpu.SMEM)],
        scratch_shapes=[
            pltpu.VMEM((TILES, 2, 8, 112, WIDE), BF16), pltpu.VMEM((4, 14, 64, D), BF16), pltpu.VMEM((T, D), BF16), pltpu.VMEM((2, 448, T), BF16),
            pltpu.VMEM((T, D), BF16), pltpu.VMEM((T, D), F32), *[pltpu.VMEM((T, WIDE), BF16)] * 3,
            pltpu.VMEM((2, 4, 112, WIDE), BF16), pltpu.VMEM((SLOTS, 2, 4, 112, WIDE), BF16), pltpu.VMEM((SLOTS, 4, 2, 64, D), BF16),
            *[pltpu.VMEM(dims, BF16) for dims in (*pair, *two, *one, *one, *one)],
            pltpu.VMEM((8, WIDE), F32), pltpu.VMEM((8, D), F32), pltpu.VMEM((8, 8, 128), F32),
            sems(6), sems(TILES + 1), sems(2, 2), *GATHER_SEMS,
            sems(3, 2), sems(3, 2), sems(8, 2), sems(8, 2), sems(4, 2), sems(4, 2), sems(3, 2), sems(3, 2), sems(2), sems(2), sems(2), sems(STEPS),
            sems(7), sems(7),
            *[pltpu.SemaphoreType.REGULAR] * 6,
        ],
        compiler_params=pltpu.CompilerParams(collective_id=1, has_side_effects=True, vmem_limit_bytes=VMEM_LIMIT),
    )(a1, a1t, h1, dy, a0t, gu, wd0, *shards)


def adamw(w, m, v, g):
    m = 0.9 * m + 0.1 * g
    v = 0.95 * v + 0.05 * g * g
    step = m * lax.rsqrt(v + 1e-8) + 0.1 * w
    return (w - 0.02 * step).astype(BF16), m, v


def solution(mesh):
    def step(x, dy, *arrays):
        weights, m, v = (arrays[i : i + 3] for i in (0, 3, 6))
        shards = (weights[0], weights[1], weights[2].reshape(2, 7, 64, D))
        gu, a0t, h1, a1, a1t, wd0, *ahead = forward(x[0], *shards)
        *gradients, squares = backward(a1, a1t, h1, dy[0], a0t, gu, wd0, *ahead, *shards)
        count = mesh.shape["s"] * sum(g.size for g in gradients)
        factor = jnp.minimum(1.0, 0.5 * lax.rsqrt(squares.reshape(()) / count + 1e-30))
        new = [adamw(w.astype(F32), m, v, g.astype(F32) * factor) for w, m, v, g in zip(weights, m, v, gradients, strict=True)]
        return tuple(one[which] for which in range(3) for one in new)

    states, cut = P(("rep", "r", "s"), None, None), P(None, "s", None)
    return jax.shard_map(
        step,
        mesh=mesh,
        in_specs=(states, states) + (cut,) * 9,
        out_specs=(P("rep", "s", None),) * 9,
        check_vma=False,
    )
```
